128 devices in a mesh: io: 64 (over z, x, y_lo, core), rep: 2 (over y_hi).
Axes of the slice: x: 4, y: 4 (y_hi: 2, y_lo: 2; y = y_hi * 2 + y_lo), z: 4, core: 2. Of those that a mesh axis runs over, the one named last changes fastest.
Arguments:
- snapshots: float32 [49152, 8192], P(('rep', 'io')), parts along dimension 0, may hold values from -6 to 6
Outputs:
- coefficients: float32 [32, 256, 8192], P('rep', None, 'io'), parts along dimension 0
- resid_var: float32 [512, 8192], P('rep', 'io'), parts along dimension 0
The draws below stay inside these ranges and needn't reach their ends.
There are 2 independent parts, one for each index of `rep`. The reference program is written for one: setup_inputs(seed, part) draws one part's arguments, and reference() takes and returns one part's arrays. A program takes and returns all parts, laid end to end along the dimension named above; each array names one. Nothing has to cross between parts.
All inputs are finite; a program needn't handle non-finite values.
Results may differ from the reference program's by a relative error of at most 0.000071.
Values sent between devices are 32-bit elements; how exact they have to be, the bound alone decides.
A program may use at most 128 MiB of HBM per device.

```python
import jax
import jax.numpy as jnp
from jax import lax

TIMES = 96
HARM = 16
LAT = 256
LON = 8192


def level_of(own_key, dims, cuts, low, top_value):
    def one(axis_at, parts):
        heights = jax.random.uniform(jax.random.fold_in(jax.random.fold_in(own_key, 6), axis_at), (parts,), jnp.float32, low / len(cuts), top_value / len(cuts))
        return jnp.repeat(jnp.exp(heights), dims[axis_at] // parts).reshape((-1,) + (1,) * (len(dims) - axis_at - 1))

    gain = one(*cuts[0])
    for cut in cuts[1:]:
        gain = gain * one(*cut)
    return gain


def normal_values(rng, dims, deviation, bound, cuts=(), dtype=jnp.bfloat16):
    array = deviation * jax.random.normal(rng, dims, jnp.float32)
    if cuts:
        array = array * level_of(rng, dims, cuts, -0.22, 0.18)
    return jnp.clip(array, -bound, bound).astype(dtype)


def setup_inputs(seed: int = 0, part: int = 0) -> dict:
    arg_keys = jax.random.split(jax.random.key(seed), 2)
    part_splits = jax.random.split(jax.random.fold_in(arg_keys[1], part), 2)
    snapshots = normal_values(part_splits[0], (TIMES * LAT, LON), 1.0, 6.0, ((0, 64),), jnp.float32)
    return {"snapshots": snapshots}


def basis_matrix(times):
    steps = jnp.arange(times).astype(jnp.float32)
    columns = [jnp.ones_like(steps), (steps - (times - 1) / 2.0) / (times / 2.0)]
    for harmonic in range(1, 7):
        columns.append(jnp.cos(2.0 * jnp.pi * harmonic * steps / 12.0))
    for harmonic in range(1, 6):
        columns.append(jnp.sin(2.0 * jnp.pi * harmonic * steps / 12.0))
    columns.append(jnp.cos(2.0 * jnp.pi * steps / times))
    columns.append(jnp.sin(2.0 * jnp.pi * steps / times))
    columns.append(jnp.cos(4.0 * jnp.pi * steps / times))
    return jnp.stack(columns, axis=1)

def projector_of(basis):
    gram = jnp.dot(basis.T, basis, precision=lax.Precision.HIGHEST)
    factor = jnp.linalg.cholesky(gram)
    middle = lax.linalg.triangular_solve(factor, basis.T, left_side=True, lower=True)
    return lax.linalg.triangular_solve(factor, middle, left_side=True, lower=True, transpose_a=True)

def reference(snapshots):
    series = snapshots.reshape(TIMES, LAT * LON)
    basis = basis_matrix(TIMES)
    projector = projector_of(basis)
    coeffs = jnp.dot(projector, series, precision=lax.Precision.HIGHEST)
    fitted = jnp.dot(basis, coeffs, precision=lax.Precision.HIGHEST)
    resid = series - fitted
    variance = jnp.mean(resid * resid, axis=0)
    return (coeffs.reshape(HARM, LAT, LON), variance.reshape(LAT, LON))
```

```python
import functools

import jax
import jax.numpy as jnp
import numpy as np
from jax import lax
from jax.experimental import pallas as pl
from jax.experimental.pallas import tpu as pltpu
from jax.sharding import PartitionSpec as P

TIMES = 96
HARM = 16
MONTHS = 12
EXTRA = 4
UNITS = 8
STAGES = 6
FLOWS = (("P", 1, 3), ("P", 3, 1), ("Q", 1, 3), ("Q", 3, 1))


def constants():
    steps = np.arange(TIMES, dtype=np.float64)
    columns = [np.ones_like(steps), (steps - (TIMES - 1) / 2.0) / (TIMES / 2.0)]
    for harmonic in range(1, 7):
        columns.append(np.cos(2.0 * np.pi * harmonic * steps / 12.0))
    for harmonic in range(1, 6):
        columns.append(np.sin(2.0 * np.pi * harmonic * steps / 12.0))
    columns.append(np.cos(2.0 * np.pi * steps / TIMES))
    columns.append(np.sin(2.0 * np.pi * steps / TIMES))
    columns.append(np.cos(4.0 * np.pi * steps / TIMES))
    basis = np.stack(columns, axis=1)
    others = (1, 13, 14, 15)
    gather = np.zeros((HARM, MONTHS + EXTRA))
    for row in range(HARM):
        if row in others:
            gather[row, MONTHS + others.index(row)] = 1.0
        else:
            gather[row, :MONTHS] = basis[:MONTHS, row]
    gram = basis.T @ basis
    fit = np.linalg.solve(gram, gather)
    root = np.linalg.cholesky(gather.T @ fit)
    table = basis[:, others]
    return table, fit, root


def flip(v, mask):
    if mask == 1:
        return v + 1 - 2 * lax.rem(v, 2)
    if mask == 3:
        return 3 - v
    return lax.rem(v + 2, 4)


def flow_shapes(kind):
    tile = (8, 128)
    if kind == "P":
        dims = {
            "own": (2, 3, 4, 2),
            "r1": (2, 3, 4, 2),
            "r2": (2, 3, 4, 2),
            "s8": (4, 2, 8),
            "r3": (2, 2, 8),
            "sum": (2, 2, 11),
            "r4": (2, 11),
            "r5": (11,),
            "out": (17,),
        }
    else:
        dims = {
            "own": (2, 3, 4, 2),
            "r1": (2, 3, 4, 2),
            "r2": (2, 3, 4, 2),
            "r3": (4, 3, 4),
            "sum": (4, 17),
            "r4": (2, 17),
            "r5": (17,),
            "out": (17,),
        }
    return {name: (UNITS,) + dim + tile for name, dim in dims.items()}


SEMS = ("ownl", "ownr", "r1", "r2", "r3", "r4", "r5")


def scratch():
    shapes = []
    for kind, _, _ in FLOWS:
        for shape in flow_shapes(kind).values():
            shapes.append(pltpu.VMEM(shape, jnp.float32))
        for _ in SEMS:
            shapes.append(pltpu.SemaphoreType.DMA((UNITS,)))
        shapes.append(pltpu.SemaphoreType.DMA((STAGES,)))
    shapes.append(pltpu.SemaphoreType.DMA((3, 2)))
    return shapes


def kernel(fit, root, table_ref, x_ref, coef_ref, var_ref, *refs):
    me = lax.axis_index("io")
    core = lax.rem(me, 2)
    y = lax.rem(lax.div(me, 2), 2)
    x = lax.rem(lax.div(me, 4), 4)
    z = lax.div(me, 16)
    parity = lax.rem(x, 2)

    def dev(zz, xx, yy, cc):
        return ((zz * 4 + xx) * 2 + yy) * 2 + cc

    refs = list(refs)
    out_sem = refs.pop()
    flows = []
    at = 0
    for number, (kind, first, second) in enumerate(FLOWS):
        flow = {"kind": kind, "f": first, "g": second, "number": number}
        for name in flow_shapes(kind):
            flow[name] = refs[at]
            at += 1
        flow["sem"] = {}
        for name in SEMS:
            flow["sem"][name] = refs[at]
            at += 1
        flow["send"] = refs[at]
        at += 1
        flows.append(flow)

    def push(src, dst, send, recv, device):
        pltpu.make_async_remote_copy(
            src_ref=src,
            dst_ref=dst,
            send_sem=send,
            recv_sem=recv,
            device_id={"io": device},
            device_id_type=pl.DeviceIdType.MESH,
        ).start()

    def await_bytes(ref, sem):
        pltpu.make_async_copy(ref, ref, sem).wait()

    barrier = pltpu.get_barrier_semaphore()
    friends = [dev(z, x, y, 1 - core), dev(z, x, 1 - y, core)]
    for mask in (1, 3):
        for c in (core, 1 - core):
            friends.append(dev(flip(z, mask), x, y, c))
            friends.append(dev(z, flip(x, mask), y, c))
    for friend in friends:
        pl.semaphore_signal(barrier, inc=1, device_id={"io": friend}, device_id_type=pl.DeviceIdType.MESH)
    pl.semaphore_wait(barrier, len(friends))

    def place(flow, i):
        return flow["number"] * (UNITS // 2) + lax.div(i, 2), lax.rem(i, 2)

    def begin(flow, i):
        lat, half = place(flow, i)
        sem = flow["sem"]
        along_z = flow["kind"] == "P"
        here = z if along_z else x
        there = flip(here, flow["f"])
        for at_home in (False, True):
            spot = here if at_home else there
            zz, xx = (spot, x) if along_z else (z, spot)
            for slot, block in ((0, spot), (1, flip(spot, flow["g"]))):
                for group, when in ((0, core), (2, core + 1), (1, 2 * core)):
                    if along_z:
                        src = x_ref.at[group, lat, block, :, :, half]
                    else:
                        src = x_ref.at[group, lat, :, block, :, half]
                    c = 1 - core if group == 1 else core
                    if not at_home:
                        push(src, flow["r1"].at[i, slot, when], flow["send"].at[0], sem["r1"].at[i], dev(zz, xx, y, c))
                    elif group == 1:
                        push(src, flow["own"].at[i, slot, when], flow["send"].at[5], sem["ownr"].at[i], dev(zz, xx, y, c))
                    else:
                        pltpu.make_async_copy(src, flow["own"].at[i, slot, when], sem["ownl"].at[i]).start()

    def second(flow, i):
        sem = flow["sem"]
        await_bytes(flow["own"].at[i, :, 0:2], sem["ownl"].at[i])
        await_bytes(flow["own"].at[i, :, 0], sem["ownr"].at[i])
        await_bytes(flow["r1"].at[i], sem["r1"].at[i])
        if flow["kind"] == "P":
            to = dev(flip(z, flow["g"]), x, y, core)
        else:
            to = dev(z, flip(x, flow["g"]), y, core)
        push(flow["own"].at[i, 1], flow["r2"].at[i, 0], flow["send"].at[1], sem["r2"].at[i], to)
        push(flow["r1"].at[i, 1], flow["r2"].at[i, 1], flow["send"].at[1], sem["r2"].at[i], to)

    def weights(chip, k):
        base = (chip * 3 + k) * EXTRA
        return [table_ref[base + j] for j in range(EXTRA)]

    def gather_stats(pieces):
        sums, moments, total = {}, [None] * EXTRA, None
        for key, k, value, w in pieces:
            sums[key, k] = value if (key, k) not in sums else sums[key, k] + value
            for j in range(EXTRA):
                term = w[j] * value
                moments[j] = term if moments[j] is None else moments[j] + term
            square = value * value
            total = square if total is None else total + square
        return sums, moments, total

    def third_p(flow, i):
        sem = flow["sem"]
        await_bytes(flow["r2"].at[i], sem["r2"].at[i])
        own, r1, r2, s8 = flow["own"], flow["r1"], flow["r2"], flow["s8"]
        f, g = flow["f"], flow["g"]
        lines = (z, flip(z, f), flip(z, g), flip(z, 2))
        for xs, xb in enumerate((x, flip(x, g), flip(x, f), flip(x, 2))):
            for ys, yb in enumerate((y, 1 - y)):
                pieces = []
                for k in range(3):
                    values = (own[i, 0, k, xb, yb], r1[i, 0, k, xb, yb], r2[i, 0, k, xb, yb], r2[i, 1, k, xb, yb])
                    for line, value in zip(lines, values):
                        pieces.append((0, k, value, weights(line * 8 + x * 2 + y, k)))
                sums, moments, total = gather_stats(pieces)
                for k in range(3):
                    s8[i, xs, ys, k] = sums[0, k]
                for j in range(EXTRA):
                    s8[i, xs, ys, 3 + j] = moments[j]
                s8[i, xs, ys, 7] = total
        push(s8.at[i, 2:4], flow["r3"].at[i], flow["send"].at[2], sem["r3"].at[i], dev(z, flip(x, f), y, core))

    def fourth_p(flow, i):
        sem = flow["sem"]
        await_bytes(flow["r3"].at[i], sem["r3"].at[i])
        s8, r3, acc = flow["s8"], flow["r3"], flow["sum"]
        for s in (1, 0):
            for ys in range(2):
                for k in range(3):
                    acc[i, s, ys, 3 * parity + k] = s8[i, s, ys, k]
                    acc[i, s, ys, 3 * (1 - parity) + k] = r3[i, s, ys, k]
                for j in range(EXTRA + 1):
                    acc[i, s, ys, 6 + j] = s8[i, s, ys, 3 + j] + r3[i, s, ys, 3 + j]
        push(acc.at[i, 1], flow["r4"].at[i], flow["send"].at[3], sem["r4"].at[i], dev(z, flip(x, flow["g"]), y, core))

    def fifth_p(flow, i):
        sem = flow["sem"]
        await_bytes(flow["r4"].at[i], sem["r4"].at[i])
        acc, r4 = flow["sum"], flow["r4"]
        for ys in (1, 0):
            acc[i, 0, ys] = acc[i, 0, ys] + r4[i, ys]
        push(acc.at[i, 0, 1], flow["r5"].at[i], flow["send"].at[4], sem["r5"].at[i], dev(z, x, 1 - y, core))

    def third_q(flow, i):
        sem = flow["sem"]
        await_bytes(flow["r2"].at[i], sem["r2"].at[i])
        to = dev(z, x, 1 - y, core)
        other = 1 - y
        r3 = flow["r3"]
        push(flow["own"].at[i, 0, :, :, other], r3.at[i, 0], flow["send"].at[2], sem["r3"].at[i], to)
        push(flow["r1"].at[i, 0, :, :, other], r3.at[i, 1], flow["send"].at[2], sem["r3"].at[i], to)
        push(flow["r2"].at[i, 0, :, :, other], r3.at[i, 2], flow["send"].at[2], sem["r3"].at[i], to)
        push(flow["r2"].at[i, 1, :, :, other], r3.at[i, 3], flow["send"].at[2], sem["r3"].at[i], to)

    def fourth_q(flow, i):
        sem = flow["sem"]
        await_bytes(flow["r3"].at[i], sem["r3"].at[i])
        own, r1, r2, r3, acc = flow["own"], flow["r1"], flow["r2"], flow["r3"], flow["sum"]
        f, g = flow["f"], flow["g"]
        spots = (x, flip(x, f), flip(x, g), flip(x, 2))
        same = (0, 1, 1, 0)
        for zs, zb in enumerate((z, flip(z, g), flip(z, f), flip(z, 2))):
            pieces = []
            for k in range(3):
                near = (own[i, 0, k, zb, y], r1[i, 0, k, zb, y], r2[i, 0, k, zb, y], r2[i, 1, k, zb, y])
                far = tuple(r3[i, s, k, zb] for s in range(4))
                for b, (values, yy) in enumerate(((near, y), (far, 1 - y))):
                    for s in range(4):
                        pieces.append(((same[s], b), k, values[s], weights(z * 8 + spots[s] * 2 + yy, k)))
            sums, moments, total = gather_stats(pieces)
            for a, xl in enumerate((parity, 1 - parity)):
                for b, yy in enumerate((y, 1 - y)):
                    for k in range(3):
                        acc[i, zs, 3 * (2 * xl + yy) + k] = sums[(a, b), k]
            for j in range(EXTRA):
                acc[i, zs, MONTHS + j] = moments[j]
            acc[i, zs, MONTHS + EXTRA] = total
        push(acc.at[i, 2:4], flow["r4"].at[i], flow["send"].at[3], sem["r4"].at[i], dev(flip(z, f), x, y, core))

    def fifth_q(flow, i):
        sem = flow["sem"]
        await_bytes(flow["r4"].at[i], sem["r4"].at[i])
        acc, r4 = flow["sum"], flow["r4"]
        for s in (1, 0):
            acc[i, s] = acc[i, s] + r4[i, s]
        push(acc.at[i, 1], flow["r5"].at[i], flow["send"].at[4], sem["r5"].at[i], dev(flip(z, flow["g"]), x, y, core))

    def finish(flow, i):
        sem = flow["sem"]
        await_bytes(flow["r5"].at[i], sem["r5"].at[i])
        acc, r5, out = flow["sum"], flow["r5"], flow["out"]
        if flow["kind"] == "P":
            w = [None] * (MONTHS + EXTRA)
            low = y == 0
            for xl in range(2):
                for k in range(3):
                    mine, theirs = acc[i, 0, 0, 3 * xl + k], r5[i, 3 * xl + k]
                    w[6 * xl + k] = jnp.where(low, mine, theirs)
                    w[6 * xl + 3 + k] = jnp.where(low, theirs, mine)
            for j in range(EXTRA):
                w[MONTHS + j] = acc[i, 0, 0, 6 + j] + r5[i, 6 + j]
            total = acc[i, 0, 0, 10] + r5[i, 10]
        else:
            w = [acc[i, 0, j] + r5[i, j] for j in range(MONTHS + EXTRA)]
            total = acc[i, 0, MONTHS + EXTRA] + r5[i, MONTHS + EXTRA]
        for row in range(HARM):
            value = None
            for j in range(MONTHS + EXTRA):
                term = w[j] * float(np.float32(fit[row, j]))
                value = term if value is None else value + term
            out[i, row] = value
        explained = None
        for col in range(HARM):
            value = None
            for j in range(col, HARM):
                if abs(root[j, col]) < 1e-12:
                    continue
                term = w[j] * float(np.float32(root[j, col]))
                value = term if value is None else value + term
            explained = value * value if explained is None else explained + value * value
        out[i, HARM] = (total - explained) * (1.0 / TIMES)
        lat, half = place(flow, i)
        row = core * 16 + lat

        @pl.when(half == core)
        def _():
            pltpu.make_async_copy(out.at[i, 0:HARM], coef_ref.at[:, row], out_sem.at[0, 0]).start()
            pltpu.make_async_copy(out.at[i, HARM], var_ref.at[row], out_sem.at[0, 1]).start()

        @pl.when(half != core)
        def _():
            to = dev(z, x, y, 1 - core)
            push(out.at[i, 0:HARM], coef_ref.at[:, row], out_sem.at[1, 0], out_sem.at[2, 0], to)
            push(out.at[i, HARM], var_ref.at[row], out_sem.at[1, 1], out_sem.at[2, 1], to)

    steps = {
        "P": (begin, second, third_p, fourth_p, fifth_p, finish),
        "Q": (begin, second, third_q, fourth_q, fifth_q, finish),
    }

    @pl.loop(0, UNITS + STAGES - 1)
    def _(turn):
        for stage in range(STAGES):
            for flow in flows:
                unit = turn - stage

                @pl.when((unit >= 0) & (unit < UNITS))
                def _(flow=flow, stage=stage, unit=unit):
                    steps[flow["kind"]][stage](flow, unit)

    for flow in flows:
        for stage in range(5):
            await_bytes(flow[f"r{stage + 1}"], flow["send"].at[stage])
        await_bytes(flow["own"].at[:, :, 0], flow["send"].at[5])
    for k in range(3):
        await_bytes(coef_ref.at[:, 0:16], out_sem.at[k, 0])
        await_bytes(var_ref.at[0:16], out_sem.at[k, 1])


def local(snapshots):
    table, fit, root = constants()
    tiles = snapshots.reshape(48, 8, 64, 128).transpose(0, 2, 1, 3)
    tiles = tiles.reshape(3, 16, 4, 4, 2, 2, 8, 128)
    coeffs, variance = pl.pallas_call(
        functools.partial(kernel, fit, root),
        out_shape=(
            jax.ShapeDtypeStruct((HARM, 32, 8, 128), jnp.float32),
            jax.ShapeDtypeStruct((32, 8, 128), jnp.float32),
        ),
        in_specs=[pl.BlockSpec(memory_space=pltpu.SMEM), pl.BlockSpec(memory_space=pl.ANY)],
        out_specs=(pl.BlockSpec(memory_space=pl.ANY), pl.BlockSpec(memory_space=pl.ANY)),
        scratch_shapes=scratch(),
        compiler_params=pltpu.CompilerParams(
            collective_id=0, has_side_effects=True, vmem_limit_bytes=60 * 1024 * 1024
        ),
    )(jnp.asarray(table.reshape(-1), dtype=jnp.float32), tiles)
    return coeffs.reshape(HARM, 256, 128), variance.reshape(256, 128)


def solution(mesh):
    return jax.shard_map(
        local,
        mesh=mesh,
        in_specs=(P(("rep", "io"), None),),
        out_specs=(P("rep", None, "io"), P("rep", "io")),
        check_vma=False,
    )
```

```python
import functools

import jax
import jax.numpy as jnp
import numpy as np
from jax import lax
from jax.experimental import pallas as pl
from jax.experimental.pallas import tpu as pltpu
from jax.sharding import PartitionSpec as P

TIMES = 96
HARM = 16
MONTHS = 12
EXTRA = 4
STAGES = 6
VMEM_LIMIT = 60817408
FLOWS = (
    ("zz", 1, "xyx", 1),
    ("zz", 3, "xxy", 3),
    ("xx", 1, "yzz", 1),
    ("xx", 3, "yzz", 3),
)
UNITS = (8, 8, 8, 8)
DELAY = (
    (6, 11, 14, 21, 26, 29),
    (7, 8, 17, 20, 29, 59),
    (5, 9, 12, 16, 26, 29),
    (6, 9, 12, 16, 20, 32),
)
KEY = (
    (20, 21, 22, 6, 0, 11),
    (3, 17, 14, 19, 13, 5),
    (23, 4, 8, 9, 2, 1),
    (7, 15, 12, 10, 18, 16),
)


def constants():
    steps = np.arange(TIMES, dtype=np.float64)
    columns = [np.ones_like(steps), (steps - (TIMES - 1) / 2.0) / (TIMES / 2.0)]
    for harmonic in range(1, 7):
        columns.append(np.cos(2.0 * np.pi * harmonic * steps / 12.0))
    for harmonic in range(1, 6):
        columns.append(np.sin(2.0 * np.pi * harmonic * steps / 12.0))
    columns.append(np.cos(2.0 * np.pi * steps / TIMES))
    columns.append(np.sin(2.0 * np.pi * steps / TIMES))
    columns.append(np.cos(4.0 * np.pi * steps / TIMES))
    basis = np.stack(columns, axis=1)
    others = (1, 13, 14, 15)
    gather = np.zeros((HARM, MONTHS + EXTRA))
    for row in range(HARM):
        if row in others:
            gather[row, MONTHS + others.index(row)] = 1.0
        else:
            gather[row, :MONTHS] = basis[:MONTHS, row]
    gram = basis.T @ basis
    fit = np.linalg.solve(gram, gather)
    root = np.linalg.cholesky(gather.T @ fit)
    table = basis[:, others]
    return table, fit, root


def flip(v, mask):
    if mask == 1:
        return v + 1 - 2 * lax.rem(v, 2)
    if mask == 3:
        return 3 - v
    return lax.rem(v + 2, 4)

def plan(flow):
    raw, _, post, _ = flow
    merged = {"x"} if raw == "xx" else set()
    values = 11 if raw == "xx" else 8
    rows = []
    for axis in post:
        joins = axis in ("x", "y") and axis not in merged
        after = values
        if joins:
            after = values + (3 if not merged else 6)
        rows.append((axis, values, after, tuple(sorted(merged)), joins))
        if joins:
            merged.add(axis)
        values = after
    return rows


def flow_shapes(number):
    units = UNITS[number]
    rows = plan(FLOWS[number])
    dims = {"own": (2, 3, 4, 2), "r1": (2, 3, 4, 2), "r2": (2, 3, 4, 2)}
    dims["s0"] = (2, 2, 2, rows[0][1])
    blocks = (2, 2, 2)
    for at, (_, before, after, _, joins) in enumerate(rows):
        blocks = blocks[1:]
        dims[f"r{at + 3}"] = blocks + (before,)
        if joins:
            dims[f"s{at + 1}"] = blocks + (after,)
    dims["out"] = (HARM + 1,)
    return {name: (units,) + dim + (8, 128) for name, dim in dims.items()}


SEMS = ("ownl", "ownr", "r1", "r2", "r3", "r4", "r5")


def scratch():
    shapes = []
    for number in range(len(FLOWS)):
        for shape in flow_shapes(number).values():
            shapes.append(pltpu.VMEM(shape, jnp.float32))
        for _ in SEMS:
            shapes.append(pltpu.SemaphoreType.DMA((UNITS[number],)))
        shapes.append(pltpu.SemaphoreType.DMA((STAGES,)))
    shapes.append(pltpu.SemaphoreType.DMA((2, 2)))
    return shapes


def kernel(fit, root, table_ref, x_ref, coef_ref, var_ref, *refs):
    me = lax.axis_index("io")
    core = lax.rem(me, 2)
    y = lax.rem(lax.div(me, 2), 2)
    x = lax.rem(lax.div(me, 4), 4)
    z = lax.div(me, 16)
    parity = lax.rem(x, 2)

    def dev(zz, xx, yy, cc):
        return ((zz * 4 + xx) * 2 + yy) * 2 + cc

    refs = list(refs)
    out_sem = refs.pop()
    flows = []
    at, base = 0, 0
    for number, spec in enumerate(FLOWS):
        raw, first, post, ring = spec
        flow = {"raw": raw, "f": first, "g": 4 - first, "post": post, "pf": ring, "pg": 4 - ring}
        flow["base"], flow["units"], flow["rows"] = base, UNITS[number], plan(spec)
        base += UNITS[number]
        for name in flow_shapes(number):
            flow[name] = refs[at]
            at += 1
        flow["sem"] = {}
        for name in SEMS:
            flow["sem"][name] = refs[at]
            at += 1
        flow["send"] = refs[at]
        at += 1
        flows.append(flow)

    def push(src, dst, send, recv, device):
        pltpu.make_async_remote_copy(
            src_ref=src,
            dst_ref=dst,
            send_sem=send,
            recv_sem=recv,
            device_id={"io": device},
            device_id_type=pl.DeviceIdType.MESH,
        ).start()

    def await_bytes(ref, sem):
        pltpu.make_async_copy(ref, ref, sem).wait()

    barrier = pltpu.get_barrier_semaphore()
    friends = [dev(z, x, y, 1 - core), dev(z, x, 1 - y, core)]
    for mask in (1, 3):
        for c in (core, 1 - core):
            friends.append(dev(flip(z, mask), x, y, c))
            friends.append(dev(z, flip(x, mask), y, c))
    for friend in friends:
        pl.semaphore_signal(barrier, inc=1, device_id={"io": friend}, device_id_type=pl.DeviceIdType.MESH)
    pl.semaphore_wait(barrier, len(friends))

    def place(flow, i):
        unit = flow["base"] + i
        return lax.div(unit, 2), lax.rem(unit, 2)

    def begin(flow, i):
        lat, half = place(flow, i)
        sem = flow["sem"]
        along_z = flow["raw"] == "zz"
        here = z if along_z else x
        there = flip(here, flow["f"])
        for at_home in (False, True):
            spot = here if at_home else there
            zz, xx = (spot, x) if along_z else (z, spot)
            for slot, block in ((0, spot), (1, flip(spot, flow["g"]))):
                for group, when in ((0, core), (2, core + 1), (1, 2 * core)):
                    if along_z:
                        src = x_ref.at[group, lat, block, :, :, half]
                    else:
                        src = x_ref.at[group, lat, :, block, :, half]
                    c = 1 - core if group == 1 else core
                    if not at_home:
                        push(src, flow["r1"].at[i, slot, when], flow["send"].at[0], sem["r1"].at[i], dev(zz, xx, y, c))
                    elif group == 1:
                        push(src, flow["own"].at[i, slot, when], flow["send"].at[5], sem["ownr"].at[i], dev(zz, xx, y, c))
                    else:
                        pltpu.make_async_copy(src, flow["own"].at[i, slot, when], sem["ownl"].at[i]).start()

    def second(flow, i):
        sem = flow["sem"]
        await_bytes(flow["own"].at[i, :, 0:2], sem["ownl"].at[i])
        await_bytes(flow["own"].at[i, :, 0], sem["ownr"].at[i])
        await_bytes(flow["r1"].at[i], sem["r1"].at[i])
        if flow["raw"] == "zz":
            to = dev(flip(z, flow["g"]), x, y, core)
        else:
            to = dev(z, flip(x, flow["g"]), y, core)
        push(flow["own"].at[i, 1], flow["r2"].at[i, 0], flow["send"].at[1], sem["r2"].at[i], to)
        push(flow["r1"].at[i, 1], flow["r2"].at[i, 1], flow["send"].at[1], sem["r2"].at[i], to)

    def partner(flow, stage):
        axis = flow["post"][stage]
        if axis == "y":
            return dev(z, x, 1 - y, core)
        mask = flow["pg"] if axis in flow["post"][:stage] else flow["pf"]
        if axis == "x":
            return dev(z, flip(x, mask), y, core)
        return dev(flip(z, mask), x, y, core)

    def send_stats(flow, i, stage, state):
        name = f"r{stage + 3}"
        push(state.at[1], flow[name].at[i], flow["send"].at[stage + 2], flow["sem"][name].at[i], partner(flow, stage))

    def weights(chip, k):
        base = (chip * 3 + k) * EXTRA
        return [table_ref[base + j] for j in range(EXTRA)]

    def reduce_raw(flow, i):
        await_bytes(flow["r2"].at[i], flow["sem"]["r2"].at[i])
        own, r1, r2, s0 = flow["own"], flow["r1"], flow["r2"], flow["s0"]
        f, g, post = flow["f"], flow["g"], flow["post"]
        along_z = flow["raw"] == "zz"
        here = z if along_z else x
        spots = (here, flip(here, f), flip(here, g), flip(here, 2))
        chips = [spot * 8 + x * 2 + y if along_z else z * 8 + spot * 2 + y for spot in spots]
        across = x if along_z else z
        ring = "x" if along_z else "z"
        for b0 in (1, 0):
            for b1 in range(2):
                for b2 in range(2):
                    bits = (b0, b1, b2)
                    lon, lon_y, seen = 0, y, False
                    for bit, axis in zip(bits, post):
                        if axis == "y":
                            lon_y = 1 - y if bit else y
                        else:
                            lon = lon ^ (bit * (flow["pg"] if seen else flow["pf"]))
                            seen = True
                    block = across if lon == 0 else flip(across, lon)
                    sums, moments, total = {}, [None] * EXTRA, None
                    for k in range(3):
                        values = (
                            own[i, 0, k, block, lon_y],
                            r1[i, 0, k, block, lon_y],
                            r2[i, 0, k, block, lon_y],
                            r2[i, 1, k, block, lon_y],
                        )
                        for number, value in enumerate(values):
                            key = (0 if along_z or number in (0, 3) else 1, k)
                            sums[key] = value if key not in sums else sums[key] + value
                            w = weights(chips[number], k)
                            for j in range(EXTRA):
                                term = w[j] * value
                                moments[j] = term if moments[j] is None else moments[j] + term
                            square = value * value
                            total = square if total is None else total + square
                    for (a, k), value in sums.items():
                        if along_z:
                            s0[i, b0, b1, b2, k] = value
                        else:
                            s0[i, b0, b1, b2, 3 * (1 - parity if a else parity) + k] = value
                    months = 3 if along_z else 6
                    for j in range(EXTRA):
                        s0[i, b0, b1, b2, months + j] = moments[j]
                    s0[i, b0, b1, b2, months + EXTRA] = total
        send_stats(flow, i, 0, s0.at[i])

    def merge(flow, i, stage):
        name = f"r{stage + 3}"
        await_bytes(flow[name].at[i], flow["sem"][name].at[i])
        axis, before, after, merged, joins = flow["rows"][stage]
        theirs = flow[name].at[i]
        mine = flow["state"].at[0]
        blocks = [()]
        for _ in range(2 - stage):
            blocks = [b + (bit,) for b in blocks for bit in (1, 0)]
        if not joins:
            for b in blocks:
                mine[b] = mine[b] + theirs[b]
            return mine
        new = flow[f"s{stage + 1}"].at[i]
        own_class = parity if axis == "x" else y
        months = before - EXTRA - 1
        for b in blocks:
            for k in range(months):
                if not merged:
                    spot = [3 * c + k for c in (own_class, 1 - own_class)]
                elif axis == "y":
                    spot = [6 * (k // 3) + 3 * c + k % 3 for c in (own_class, 1 - own_class)]
                else:
                    spot = [6 * c + k for c in (own_class, 1 - own_class)]
                new[b + (spot[0],)] = mine[b + (k,)]
                new[b + (spot[1],)] = theirs[b + (k,)]
            for j in range(EXTRA + 1):
                new[b + (2 * months + j,)] = mine[b + (months + j,)] + theirs[b + (months + j,)]
        return new

    def exchange(flow, i, stage):
        flow["state"] = flow["s0"].at[i]
        for done in range(stage - 1):
            joins = flow["rows"][done][4]
            flow["state"] = flow[f"s{done + 1}"].at[i] if joins else flow["state"].at[0]
        state = merge(flow, i, stage - 1)
        if stage < 3:
            send_stats(flow, i, stage, state)
        return state

    def finish(flow, i):
        state = exchange(flow, i, 3)
        out = flow["out"]
        w = [state[j] for j in range(MONTHS + EXTRA)]
        total = state[MONTHS + EXTRA]
        for row in range(HARM):
            value = None
            for j in range(MONTHS + EXTRA):
                term = w[j] * float(np.float32(fit[row, j]))
                value = term if value is None else value + term
            out[i, row] = value
        explained = None
        for col in range(HARM):
            value = None
            for j in range(col, HARM):
                if abs(root[j, col]) < 1e-12:
                    continue
                term = w[j] * float(np.float32(root[j, col]))
                value = term if value is None else value + term
            explained = value * value if explained is None else explained + value * value
        out[i, HARM] = (total - explained) * (1.0 / TIMES)
        lat, half = place(flow, i)
        row = core * 16 + lat

        @pl.when(half != core)
        def _():
            to = dev(z, x, y, 1 - core)
            push(out.at[i, 0:HARM], coef_ref.at[:, row], out_sem.at[0, 0], out_sem.at[1, 0], to)
            push(out.at[i, HARM], var_ref.at[row], out_sem.at[0, 1], out_sem.at[1, 1], to)

        @pl.when(half == core)
        def _():
            for k in range(HARM):
                coef_ref[k, row] = out[i, k]
            var_ref[row] = out[i, HARM]

    def step(flow, stage, i):
        if stage == 0:
            begin(flow, i)
        elif stage == 1:
            second(flow, i)
        elif stage == 2:
            reduce_raw(flow, i)
        elif stage == 5:
            finish(flow, i)
        else:
            exchange(flow, i, stage - 2)

    order = sorted((KEY[f][s], f, s) for f in range(len(FLOWS)) for s in range(STAGES))

    @pl.loop(0, max(u + max(d) for u, d in zip(UNITS, DELAY)))
    def _(turn):
        for _, number, stage in order:
            flow = flows[number]
            unit = turn - DELAY[number][stage]

            @pl.when((unit >= 0) & (unit < flow["units"]))
            def _(flow=flow, stage=stage, unit=unit):
                step(flow, stage, unit)

    for flow in flows:
        for stage in range(5):
            await_bytes(flow[f"r{stage + 1}"], flow["send"].at[stage])
        await_bytes(flow["own"].at[:, :, 0], flow["send"].at[5])
    for k in range(2):
        await_bytes(coef_ref.at[:, 0:16], out_sem.at[k, 0])
        await_bytes(var_ref.at[0:16], out_sem.at[k, 1])


def local(snapshots):
    table, fit, root = constants()
    tiles = snapshots.reshape(48, 8, 64, 128).transpose(0, 2, 1, 3)
    tiles = tiles.reshape(3, 16, 4, 4, 2, 2, 8, 128)
    coeffs, variance = pl.pallas_call(
        functools.partial(kernel, fit, root),
        out_shape=(
            pltpu.VMEM((HARM, 32, 8, 128), jnp.float32),
            pltpu.VMEM((32, 8, 128), jnp.float32),
        ),
        in_specs=[pl.BlockSpec(memory_space=pltpu.SMEM), pl.BlockSpec(memory_space=pl.ANY)],
        out_specs=(pl.BlockSpec(memory_space=pltpu.VMEM), pl.BlockSpec(memory_space=pltpu.VMEM)),
        scratch_shapes=scratch(),
        compiler_params=pltpu.CompilerParams(
            collective_id=0, has_side_effects=True, vmem_limit_bytes=VMEM_LIMIT
        ),
    )(jnp.asarray(table.reshape(-1), dtype=jnp.float32), tiles)
    return coeffs.reshape(HARM, 256, 128), variance.reshape(256, 128)


def solution(mesh):
    return jax.shard_map(
        local,
        mesh=mesh,
        in_specs=(P(("rep", "io"), None),),
        out_specs=(P("rep", None, "io"), P("rep", "io")),
        check_vma=False,
    )
```

```python
import functools

import jax
import jax.numpy as jnp
import numpy as np
from jax import lax
from jax.experimental import pallas as pl
from jax.experimental.pallas import tpu as pltpu
from jax.sharding import PartitionSpec as P

TIMES = 96
HARM = 16
MONTHS = 12
EXTRA = 4
STAGES = 6
VMEM_LIMIT = 60817408
FLOWS = (
    ("zz", 1, "xyx", 1),
    ("zz", 3, "xyx", 3),
    ("zz", 1, "xxy", 1),
    ("zz", 3, "xxy", 3),
    ("xx", 1, "yzz", 1),
    ("xx", 3, "yzz", 3),
)
UNITS = (4, 4, 4, 4, 8, 8)
DELAY = (
    (1, 3, 9, 12, 16, 19),
    (1, 4, 8, 10, 14, 18),
    (2, 6, 10, 13, 15, 18),
    (0, 8, 10, 13, 16, 19),
    (1, 3, 5, 8, 11, 14),
    (0, 3, 4, 7, 11, 14),
)
KEY = (
    (10, 34, 32, 20, 2, 3),
    (25, 19, 26, 16, 24, 17),
    (21, 18, 0, 1, 15, 6),
    (35, 7, 28, 13, 22, 33),
    (5, 14, 8, 12, 27, 30),
    (23, 4, 31, 29, 9, 11),
)


def constants():
    steps = np.arange(TIMES, dtype=np.float64)
    columns = [np.ones_like(steps), (steps - (TIMES - 1) / 2.0) / (TIMES / 2.0)]
    for harmonic in range(1, 7):
        columns.append(np.cos(2.0 * np.pi * harmonic * steps / 12.0))
    for harmonic in range(1, 6):
        columns.append(np.sin(2.0 * np.pi * harmonic * steps / 12.0))
    columns.append(np.cos(2.0 * np.pi * steps / TIMES))
    columns.append(np.sin(2.0 * np.pi * steps / TIMES))
    columns.append(np.cos(4.0 * np.pi * steps / TIMES))
    basis = np.stack(columns, axis=1)
    others = (1, 13, 14, 15)
    gather = np.zeros((HARM, MONTHS + EXTRA))
    for row in range(HARM):
        if row in others:
            gather[row, MONTHS + others.index(row)] = 1.0
        else:
            gather[row, :MONTHS] = basis[:MONTHS, row]
    gram = basis.T @ basis
    fit = np.linalg.solve(gram, gather)
    root = np.linalg.cholesky(gather.T @ fit)
    table = basis[:, others]
    return table, fit, root


def flip(v, mask):
    if mask == 1:
        return v + 1 - 2 * lax.rem(v, 2)
    if mask == 3:
        return 3 - v
    return lax.rem(v + 2, 4)

def plan(flow):
    raw, _, post, _ = flow
    merged = {"x"} if raw == "xx" else set()
    values = 11 if raw == "xx" else 8
    rows = []
    for axis in post:
        joins = axis in ("x", "y") and axis not in merged
        after = values
        if joins:
            after = values + (3 if not merged else 6)
        rows.append((axis, values, after, tuple(sorted(merged)), joins))
        if joins:
            merged.add(axis)
        values = after
    return rows


def flow_shapes(number):
    units = UNITS[number]
    rows = plan(FLOWS[number])
    dims = {"own": (2, 3, 4, 2), "r1": (2, 3, 4, 2), "r2": (2, 3, 4, 2)}
    dims["s0"] = (2, 2, 2, rows[0][1])
    blocks = (2, 2, 2)
    for at, (_, before, after, _, joins) in enumerate(rows):
        blocks = blocks[1:]
        dims[f"r{at + 3}"] = blocks + (before,)
        if joins:
            dims[f"s{at + 1}"] = blocks + (after,)
    dims["out"] = (HARM + 1,)
    return {name: (units,) + dim + (8, 128) for name, dim in dims.items()}


SEMS = ("ownl", "ownr", "r1", "r2", "r3", "r4", "r5")


def scratch():
    shapes = []
    for number in range(len(FLOWS)):
        for shape in flow_shapes(number).values():
            shapes.append(pltpu.VMEM(shape, jnp.float32))
        for _ in SEMS:
            shapes.append(pltpu.SemaphoreType.DMA((UNITS[number],)))
        shapes.append(pltpu.SemaphoreType.DMA((STAGES,)))
    shapes.append(pltpu.SemaphoreType.DMA((2, 2)))
    return shapes


def kernel(fit, root, table_ref, x_ref, coef_ref, var_ref, *refs):
    me = lax.axis_index("io")
    core = lax.rem(me, 2)
    y = lax.rem(lax.div(me, 2), 2)
    x = lax.rem(lax.div(me, 4), 4)
    z = lax.div(me, 16)
    parity = lax.rem(x, 2)

    def dev(zz, xx, yy, cc):
        return ((zz * 4 + xx) * 2 + yy) * 2 + cc

    refs = list(refs)
    out_sem = refs.pop()
    flows = []
    at, base = 0, 0
    for number, spec in enumerate(FLOWS):
        raw, first, post, ring = spec
        flow = {"raw": raw, "f": first, "g": 4 - first, "post": post, "pf": ring, "pg": 4 - ring}
        flow["base"], flow["units"], flow["rows"] = base, UNITS[number], plan(spec)
        base += UNITS[number]
        for name in flow_shapes(number):
            flow[name] = refs[at]
            at += 1
        flow["sem"] = {}
        for name in SEMS:
            flow["sem"][name] = refs[at]
            at += 1
        flow["send"] = refs[at]
        at += 1
        flows.append(flow)

    def push(src, dst, send, recv, device):
        pltpu.make_async_remote_copy(
            src_ref=src,
            dst_ref=dst,
            send_sem=send,
            recv_sem=recv,
            device_id={"io": device},
            device_id_type=pl.DeviceIdType.MESH,
        ).start()

    def await_bytes(ref, sem):
        pltpu.make_async_copy(ref, ref, sem).wait()

    barrier = pltpu.get_barrier_semaphore()
    friends = [dev(z, x, y, 1 - core), dev(z, x, 1 - y, core)]
    for mask in (1, 3):
        for c in (core, 1 - core):
            friends.append(dev(flip(z, mask), x, y, c))
            friends.append(dev(z, flip(x, mask), y, c))
    for friend in friends:
        pl.semaphore_signal(barrier, inc=1, device_id={"io": friend}, device_id_type=pl.DeviceIdType.MESH)
    pl.semaphore_wait(barrier, len(friends))

    def place(flow, i):
        unit = flow["base"] + i
        return lax.div(unit, 2), lax.rem(unit, 2)

    def begin(flow, i):
        lat, half = place(flow, i)
        sem = flow["sem"]
        along_z = flow["raw"] == "zz"
        here = z if along_z else x
        there = flip(here, flow["f"])
        for at_home in (False, True):
            spot = here if at_home else there
            zz, xx = (spot, x) if along_z else (z, spot)
            for slot, block in ((0, spot), (1, flip(spot, flow["g"]))):
                for group, when in ((0, core), (2, core + 1), (1, 2 * core)):
                    if along_z:
                        src = x_ref.at[group, lat, block, :, :, half]
                    else:
                        src = x_ref.at[group, lat, :, block, :, half]
                    c = 1 - core if group == 1 else core
                    if not at_home:
                        push(src, flow["r1"].at[i, slot, when], flow["send"].at[0], sem["r1"].at[i], dev(zz, xx, y, c))
                    elif group == 1:
                        push(src, flow["own"].at[i, slot, when], flow["send"].at[5], sem["ownr"].at[i], dev(zz, xx, y, c))
                    else:
                        pltpu.make_async_copy(src, flow["own"].at[i, slot, when], sem["ownl"].at[i]).start()

    def second(flow, i):
        sem = flow["sem"]
        await_bytes(flow["own"].at[i, :, 0:2], sem["ownl"].at[i])
        await_bytes(flow["own"].at[i, :, 0], sem["ownr"].at[i])
        await_bytes(flow["r1"].at[i], sem["r1"].at[i])
        if flow["raw"] == "zz":
            to = dev(flip(z, flow["g"]), x, y, core)
        else:
            to = dev(z, flip(x, flow["g"]), y, core)
        push(flow["own"].at[i, 1], flow["r2"].at[i, 0], flow["send"].at[1], sem["r2"].at[i], to)
        push(flow["r1"].at[i, 1], flow["r2"].at[i, 1], flow["send"].at[1], sem["r2"].at[i], to)

    def partner(flow, stage):
        axis = flow["post"][stage]
        if axis == "y":
            return dev(z, x, 1 - y, core)
        mask = flow["pg"] if axis in flow["post"][:stage] else flow["pf"]
        if axis == "x":
            return dev(z, flip(x, mask), y, core)
        return dev(flip(z, mask), x, y, core)

    def send_stats(flow, i, stage, state):
        name = f"r{stage + 3}"
        push(state.at[1], flow[name].at[i], flow["send"].at[stage + 2], flow["sem"][name].at[i], partner(flow, stage))

    def weights(chip, k):
        base = (chip * 3 + k) * EXTRA
        return [table_ref[base + j] for j in range(EXTRA)]

    def reduce_raw(flow, i):
        await_bytes(flow["r2"].at[i], flow["sem"]["r2"].at[i])
        own, r1, r2, s0 = flow["own"], flow["r1"], flow["r2"], flow["s0"]
        f, g, post = flow["f"], flow["g"], flow["post"]
        along_z = flow["raw"] == "zz"
        here = z if along_z else x
        spots = (here, flip(here, f), flip(here, g), flip(here, 2))
        chips = [spot * 8 + x * 2 + y if along_z else z * 8 + spot * 2 + y for spot in spots]
        across = x if along_z else z
        ring = "x" if along_z else "z"
        for b0 in (1, 0):
            for b1 in range(2):
                for b2 in range(2):
                    bits = (b0, b1, b2)
                    lon, lon_y, seen = 0, y, False
                    for bit, axis in zip(bits, post):
                        if axis == "y":
                            lon_y = 1 - y if bit else y
                        else:
                            lon = lon ^ (bit * (flow["pg"] if seen else flow["pf"]))
                            seen = True
                    block = across if lon == 0 else flip(across, lon)
                    sums, moments, total = {}, [None] * EXTRA, None
                    for k in range(3):
                        values = (
                            own[i, 0, k, block, lon_y],
                            r1[i, 0, k, block, lon_y],
                            r2[i, 0, k, block, lon_y],
                            r2[i, 1, k, block, lon_y],
                        )
                        for number, value in enumerate(values):
                            key = (0 if along_z or number in (0, 3) else 1, k)
                            sums[key] = value if key not in sums else sums[key] + value
                            w = weights(chips[number], k)
                            for j in range(EXTRA):
                                term = w[j] * value
                                moments[j] = term if moments[j] is None else moments[j] + term
                            square = value * value
                            total = square if total is None else total + square
                    for (a, k), value in sums.items():
                        if along_z:
                            s0[i, b0, b1, b2, k] = value
                        else:
                            s0[i, b0, b1, b2, 3 * (1 - parity if a else parity) + k] = value
                    months = 3 if along_z else 6
                    for j in range(EXTRA):
                        s0[i, b0, b1, b2, months + j] = moments[j]
                    s0[i, b0, b1, b2, months + EXTRA] = total
        send_stats(flow, i, 0, s0.at[i])

    def merge(flow, i, stage):
        name = f"r{stage + 3}"
        await_bytes(flow[name].at[i], flow["sem"][name].at[i])
        axis, before, after, merged, joins = flow["rows"][stage]
        theirs = flow[name].at[i]
        mine = flow["state"].at[0]
        blocks = [()]
        for _ in range(2 - stage):
            blocks = [b + (bit,) for b in blocks for bit in (1, 0)]
        if not joins:
            for b in blocks:
                mine[b] = mine[b] + theirs[b]
            return mine
        new = flow[f"s{stage + 1}"].at[i]
        own_class = parity if axis == "x" else y
        months = before - EXTRA - 1
        for b in blocks:
            for k in range(months):
                if not merged:
                    spot = [3 * c + k for c in (own_class, 1 - own_class)]
                elif axis == "y":
                    spot = [6 * (k // 3) + 3 * c + k % 3 for c in (own_class, 1 - own_class)]
                else:
                    spot = [6 * c + k for c in (own_class, 1 - own_class)]
                new[b + (spot[0],)] = mine[b + (k,)]
                new[b + (spot[1],)] = theirs[b + (k,)]
            for j in range(EXTRA + 1):
                new[b + (2 * months + j,)] = mine[b + (months + j,)] + theirs[b + (months + j,)]
        return new

    def exchange(flow, i, stage):
        flow["state"] = flow["s0"].at[i]
        for done in range(stage - 1):
            joins = flow["rows"][done][4]
            flow["state"] = flow[f"s{done + 1}"].at[i] if joins else flow["state"].at[0]
        state = merge(flow, i, stage - 1)
        if stage < 3:
            send_stats(flow, i, stage, state)
        return state

    def finish(flow, i):
        state = exchange(flow, i, 3)
        out = flow["out"]
        w = [state[j] for j in range(MONTHS + EXTRA)]
        total = state[MONTHS + EXTRA]
        for row in range(HARM):
            value = None
            for j in range(MONTHS + EXTRA):
                term = w[j] * float(np.float32(fit[row, j]))
                value = term if value is None else value + term
            out[i, row] = value
        explained = None
        for col in range(HARM):
            value = None
            for j in range(col, HARM):
                if abs(root[j, col]) < 1e-12:
                    continue
                term = w[j] * float(np.float32(root[j, col]))
                value = term if value is None else value + term
            explained = value * value if explained is None else explained + value * value
        out[i, HARM] = (total - explained) * (1.0 / TIMES)
        lat, half = place(flow, i)
        row = core * 16 + lat

        @pl.when(half != core)
        def _():
            to = dev(z, x, y, 1 - core)
            push(out.at[i, 0:HARM], coef_ref.at[:, row], out_sem.at[0, 0], out_sem.at[1, 0], to)
            push(out.at[i, HARM], var_ref.at[row], out_sem.at[0, 1], out_sem.at[1, 1], to)

        @pl.when(half == core)
        def _():
            for k in range(HARM):
                coef_ref[k, row] = out[i, k]
            var_ref[row] = out[i, HARM]

    def step(flow, stage, i):
        if stage == 0:
            begin(flow, i)
        elif stage == 1:
            second(flow, i)
        elif stage == 2:
            reduce_raw(flow, i)
        elif stage == 5:
            finish(flow, i)
        else:
            exchange(flow, i, stage - 2)

    order = sorted((KEY[f][s], f, s) for f in range(len(FLOWS)) for s in range(STAGES))

    @pl.loop(0, max(u + max(d) for u, d in zip(UNITS, DELAY)))
    def _(turn):
        for _, number, stage in order:
            flow = flows[number]
            unit = turn - DELAY[number][stage]

            @pl.when((unit >= 0) & (unit < flow["units"]))
            def _(flow=flow, stage=stage, unit=unit):
                step(flow, stage, unit)

    for flow in flows:
        for stage in range(5):
            await_bytes(flow[f"r{stage + 1}"], flow["send"].at[stage])
        await_bytes(flow["own"].at[:, :, 0], flow["send"].at[5])
    for k in range(2):
        await_bytes(coef_ref.at[:, 0:16], out_sem.at[k, 0])
        await_bytes(var_ref.at[0:16], out_sem.at[k, 1])


def local(snapshots):
    table, fit, root = constants()
    tiles = snapshots.reshape(48, 8, 64, 128).transpose(0, 2, 1, 3)
    tiles = tiles.reshape(3, 16, 4, 4, 2, 2, 8, 128)
    coeffs, variance = pl.pallas_call(
        functools.partial(kernel, fit, root),
        out_shape=(
            pltpu.VMEM((HARM, 32, 8, 128), jnp.float32),
            pltpu.VMEM((32, 8, 128), jnp.float32),
        ),
        in_specs=[pl.BlockSpec(memory_space=pltpu.SMEM), pl.BlockSpec(memory_space=pl.ANY)],
        out_specs=(pl.BlockSpec(memory_space=pltpu.VMEM), pl.BlockSpec(memory_space=pltpu.VMEM)),
        scratch_shapes=scratch(),
        compiler_params=pltpu.CompilerParams(
            collective_id=0, has_side_effects=True, vmem_limit_bytes=VMEM_LIMIT
        ),
    )(jnp.asarray(table.reshape(-1), dtype=jnp.float32), tiles)
    return coeffs.reshape(HARM, 256, 128), variance.reshape(256, 128)


def solution(mesh):
    return jax.shard_map(
        local,
        mesh=mesh,
        in_specs=(P(("rep", "io"), None),),
        out_specs=(P("rep", None, "io"), P("rep", "io")),
        check_vma=False,
    )
```

```python
import functools

import jax
import jax.numpy as jnp
import numpy as np
from jax import lax
from jax.experimental import pallas as pl
from jax.experimental.pallas import tpu as pltpu
from jax.sharding import PartitionSpec as P

TIMES = 96
HARM = 16
MONTHS = 12
EXTRA = 4
STAGES = 6
VMEM_LIMIT = 60817408
FLOWS = (
    ("zz", 1, "xxy", 1),
    ("zz", 3, "xxy", 3),
    ("zz", 1, "yxx", 1),
    ("zz", 3, "yxx", 3),
    ("xx", 1, "yzz", 1),
    ("xx", 3, "yzz", 3),
)
UNITS = (6, 6, 2, 2, 8, 8)
DELAY = (
    (1, 5, 8, 11, 14, 17),
    (1, 6, 9, 11, 13, 16),
    (1, 3, 5, 14, 17, 20),
    (1, 5, 11, 15, 17, 20),
    (0, 2, 4, 8, 11, 15),
    (1, 3, 4, 8, 11, 15),
)
KEY = (
    (31, 28, 16, 27, 9, 7),
    (32, 23, 4, 5, 35, 11),
    (12, 26, 29, 22, 18, 13),
    (1, 14, 19, 8, 30, 10),
    (21, 33, 24, 15, 20, 3),
    (0, 6, 34, 17, 25, 2),
)


def constants():
    steps = np.arange(TIMES, dtype=np.float64)
    columns = [np.ones_like(steps), (steps - (TIMES - 1) / 2.0) / (TIMES / 2.0)]
    for harmonic in range(1, 7):
        columns.append(np.cos(2.0 * np.pi * harmonic * steps / 12.0))
    for harmonic in range(1, 6):
        columns.append(np.sin(2.0 * np.pi * harmonic * steps / 12.0))
    columns.append(np.cos(2.0 * np.pi * steps / TIMES))
    columns.append(np.sin(2.0 * np.pi * steps / TIMES))
    columns.append(np.cos(4.0 * np.pi * steps / TIMES))
    basis = np.stack(columns, axis=1)
    others = (1, 13, 14, 15)
    gather = np.zeros((HARM, MONTHS + EXTRA))
    for row in range(HARM):
        if row in others:
            gather[row, MONTHS + others.index(row)] = 1.0
        else:
            gather[row, :MONTHS] = basis[:MONTHS, row]
    gram = basis.T @ basis
    fit = np.linalg.solve(gram, gather)
    root = np.linalg.cholesky(gather.T @ fit)
    table = basis[:, others]
    return table, fit, root


def flip(v, mask):
    if mask == 1:
        return v + 1 - 2 * lax.rem(v, 2)
    if mask == 3:
        return 3 - v
    return lax.rem(v + 2, 4)

def plan(flow):
    raw, _, post, _ = flow
    merged = {"x"} if raw == "xx" else set()
    values = 11 if raw == "xx" else 8
    rows = []
    for axis in post:
        joins = axis in ("x", "y") and axis not in merged
        after = values
        if joins:
            after = values + (3 if not merged else 6)
        rows.append((axis, values, after, tuple(sorted(merged)), joins))
        if joins:
            merged.add(axis)
        values = after
    return rows


def flow_shapes(number):
    units = UNITS[number]
    rows = plan(FLOWS[number])
    dims = {"r1": (2, 2, 3, 4, 2), "r2": (2, 3, 4, 2)}
    dims["s0"] = (2, 2, 2, rows[0][1])
    blocks = (2, 2, 2)
    for at, (_, before, after, _, joins) in enumerate(rows):
        blocks = blocks[1:]
        dims[f"r{at + 3}"] = blocks + (before,)
        if joins:
            dims[f"s{at + 1}"] = blocks + (after,)
    dims["out"] = (HARM + 1,)
    return {name: (units,) + dim + (8, 128) for name, dim in dims.items()}


SEMS = ("r1", "r2", "r3", "r4", "r5")


def scratch():
    shapes = []
    for number in range(len(FLOWS)):
        for shape in flow_shapes(number).values():
            shapes.append(pltpu.VMEM(shape, jnp.float32))
        for _ in SEMS:
            shapes.append(pltpu.SemaphoreType.DMA((UNITS[number],)))
    shapes.append(pltpu.SemaphoreType.DMA((STAGES,)))
    shapes.append(pltpu.SMEM((TIMES * EXTRA,), jnp.float32))
    shapes.append(pltpu.SemaphoreType.DMA(()))
    shapes.append(pltpu.SemaphoreType.DMA((2, 2)))
    return shapes


def kernel(fit, root, table_hbm, x_ref, coef_ref, var_ref, *refs):
    me = lax.axis_index("io")
    core = lax.rem(me, 2)
    y = lax.rem(lax.div(me, 2), 2)
    x = lax.rem(lax.div(me, 4), 4)
    z = lax.div(me, 16)
    parity = lax.rem(x, 2)

    def dev(zz, xx, yy, cc):
        return ((zz * 4 + xx) * 2 + yy) * 2 + cc

    refs = list(refs)
    out_sem = refs.pop()
    table_sem = refs.pop()
    table_ref = refs.pop()
    send = refs.pop()
    table_copy = pltpu.make_async_copy(table_hbm, table_ref, table_sem)
    table_copy.start()
    flows = []
    at, base = 0, 0
    for number, spec in enumerate(FLOWS):
        raw, first, post, ring = spec
        flow = {"raw": raw, "f": first, "g": 4 - first, "post": post, "pf": ring, "pg": 4 - ring}
        flow["base"], flow["units"], flow["rows"] = base, UNITS[number], plan(spec)
        base += UNITS[number]
        for name in flow_shapes(number):
            flow[name] = refs[at]
            at += 1
        flow["sem"] = {}
        for name in SEMS:
            flow["sem"][name] = refs[at]
            at += 1
        flows.append(flow)

    def push(src, dst, send, recv, device):
        pltpu.make_async_remote_copy(
            src_ref=src,
            dst_ref=dst,
            send_sem=send,
            recv_sem=recv,
            device_id={"io": device},
            device_id_type=pl.DeviceIdType.MESH,
        ).start()

    def await_bytes(ref, sem):
        pltpu.make_async_copy(ref, ref, sem).wait()

    barrier = pltpu.get_barrier_semaphore()
    friends = [dev(z, x, y, 1 - core), dev(z, x, 1 - y, core)]
    for mask in (1, 3):
        for c in (core, 1 - core):
            friends.append(dev(flip(z, mask), x, y, c))
            friends.append(dev(z, flip(x, mask), y, c))
    for friend in friends:
        pl.semaphore_signal(barrier, inc=1, device_id={"io": friend}, device_id_type=pl.DeviceIdType.MESH)
    pl.semaphore_wait(barrier, len(friends))

    def place(flow, i):
        unit = flow["base"] + i
        return lax.div(unit, 2), lax.rem(unit, 2)

    def begin(flow, i):
        lat, half = place(flow, i)
        sem = flow["sem"]
        along_z = flow["raw"] == "zz"
        here = z if along_z else x
        there = flip(here, flow["f"])
        for at_home in (False, True):
            spot = here if at_home else there
            zz, xx = (spot, x) if along_z else (z, spot)
            for slot, block in ((0, spot), (1, flip(spot, flow["g"]))):
                for group, when in ((0, core), (2, core + 1), (1, 2 * core)):
                    if along_z:
                        src = x_ref.at[group, lat, block, :, :, half]
                    else:
                        src = x_ref.at[group, lat, :, block, :, half]
                    c = 1 - core if group == 1 else core
                    if not at_home:
                        push(src, flow["r1"].at[i, 1, slot, when], send.at[0], sem["r1"].at[i], dev(zz, xx, y, c))
                    elif group == 1:
                        push(src, flow["r1"].at[i, 0, slot, when], send.at[1], sem["r1"].at[i], dev(zz, xx, y, c))
                    else:
                        pltpu.make_async_copy(src, flow["r1"].at[i, 0, slot, when], sem["r1"].at[i]).start()

    def second(flow, i):
        sem = flow["sem"]
        await_bytes(flow["r1"].at[i], sem["r1"].at[i])
        if flow["raw"] == "zz":
            to = dev(flip(z, flow["g"]), x, y, core)
        else:
            to = dev(z, flip(x, flow["g"]), y, core)
        push(flow["r1"].at[i, 0, 1], flow["r2"].at[i, 0], send.at[2], sem["r2"].at[i], to)
        push(flow["r1"].at[i, 1, 1], flow["r2"].at[i, 1], send.at[2], sem["r2"].at[i], to)

    def partner(flow, stage):
        axis = flow["post"][stage]
        if axis == "y":
            return dev(z, x, 1 - y, core)
        mask = flow["pg"] if axis in flow["post"][:stage] else flow["pf"]
        if axis == "x":
            return dev(z, flip(x, mask), y, core)
        return dev(flip(z, mask), x, y, core)

    def send_stats(flow, i, stage, state):
        name = f"r{stage + 3}"
        push(state.at[1], flow[name].at[i], send.at[stage + 3], flow["sem"][name].at[i], partner(flow, stage))

    def weights(chip, k):
        base = (chip * 3 + k) * EXTRA
        return [table_ref[base + j] for j in range(EXTRA)]

    def reduce_raw(flow, i):
        await_bytes(flow["r2"].at[i], flow["sem"]["r2"].at[i])
        r1, r2, s0 = flow["r1"], flow["r2"], flow["s0"]
        f, g, post = flow["f"], flow["g"], flow["post"]
        along_z = flow["raw"] == "zz"
        here = z if along_z else x
        spots = (here, flip(here, f), flip(here, g), flip(here, 2))
        chips = [spot * 8 + x * 2 + y if along_z else z * 8 + spot * 2 + y for spot in spots]
        across = x if along_z else z
        ring = "x" if along_z else "z"
        for b0 in (1, 0):
            for b1 in range(2):
                for b2 in range(2):
                    bits = (b0, b1, b2)
                    lon, lon_y, seen = 0, y, False
                    for bit, axis in zip(bits, post):
                        if axis == "y":
                            lon_y = 1 - y if bit else y
                        else:
                            lon = lon ^ (bit * (flow["pg"] if seen else flow["pf"]))
                            seen = True
                    block = across if lon == 0 else flip(across, lon)
                    sums, moments, total = {}, [None] * EXTRA, None
                    for k in range(3):
                        values = (
                            r1[i, 0, 0, k, block, lon_y],
                            r1[i, 1, 0, k, block, lon_y],
                            r2[i, 0, k, block, lon_y],
                            r2[i, 1, k, block, lon_y],
                        )
                        for number, value in enumerate(values):
                            key = (0 if along_z or number in (0, 3) else 1, k)
                            sums[key] = value if key not in sums else sums[key] + value
                            w = weights(chips[number], k)
                            for j in range(EXTRA):
                                term = w[j] * value
                                moments[j] = term if moments[j] is None else moments[j] + term
                            square = value * value
                            total = square if total is None else total + square
                    for (a, k), value in sums.items():
                        if along_z:
                            s0[i, b0, b1, b2, k] = value
                        else:
                            s0[i, b0, b1, b2, 3 * (1 - parity if a else parity) + k] = value
                    months = 3 if along_z else 6
                    for j in range(EXTRA):
                        s0[i, b0, b1, b2, months + j] = moments[j]
                    s0[i, b0, b1, b2, months + EXTRA] = total
        send_stats(flow, i, 0, s0.at[i])

    def merge(flow, i, stage):
        name = f"r{stage + 3}"
        await_bytes(flow[name].at[i], flow["sem"][name].at[i])
        axis, before, after, merged, joins = flow["rows"][stage]
        theirs = flow[name].at[i]
        mine = flow["state"].at[0]
        blocks = [()]
        for _ in range(2 - stage):
            blocks = [b + (bit,) for b in blocks for bit in (1, 0)]
        if not joins:
            for b in blocks:
                mine[b] = mine[b] + theirs[b]
            return mine
        new = flow[f"s{stage + 1}"].at[i]
        own_class = parity if axis == "x" else y
        months = before - EXTRA - 1
        for b in blocks:
            for k in range(months):
                if not merged:
                    spot = [3 * c + k for c in (own_class, 1 - own_class)]
                elif axis == "y":
                    spot = [6 * (k // 3) + 3 * c + k % 3 for c in (own_class, 1 - own_class)]
                else:
                    spot = [6 * c + k for c in (own_class, 1 - own_class)]
                new[b + (spot[0],)] = mine[b + (k,)]
                new[b + (spot[1],)] = theirs[b + (k,)]
            for j in range(EXTRA + 1):
                new[b + (2 * months + j,)] = mine[b + (months + j,)] + theirs[b + (months + j,)]
        return new

    def exchange(flow, i, stage):
        flow["state"] = flow["s0"].at[i]
        for done in range(stage - 1):
            joins = flow["rows"][done][4]
            flow["state"] = flow[f"s{done + 1}"].at[i] if joins else flow["state"].at[0]
        state = merge(flow, i, stage - 1)
        if stage < 3:
            send_stats(flow, i, stage, state)
        return state

    def finish(flow, i):
        state = exchange(flow, i, 3)
        out = flow["out"]
        w = [state[j] for j in range(MONTHS + EXTRA)]
        total = state[MONTHS + EXTRA]
        for row in range(HARM):
            value = None
            for j in range(MONTHS + EXTRA):
                term = w[j] * float(np.float32(fit[row, j]))
                value = term if value is None else value + term
            out[i, row] = value
        explained = None
        for col in range(HARM):
            value = None
            for j in range(col, HARM):
                if abs(root[j, col]) < 1e-12:
                    continue
                term = w[j] * float(np.float32(root[j, col]))
                value = term if value is None else value + term
            explained = value * value if explained is None else explained + value * value
        out[i, HARM] = (total - explained) * (1.0 / TIMES)
        lat, half = place(flow, i)
        row = core * 16 + lat

        @pl.when(half != core)
        def _():
            to = dev(z, x, y, 1 - core)
            push(out.at[i, 0:HARM], coef_ref.at[:, row], out_sem.at[0, 0], out_sem.at[1, 0], to)
            push(out.at[i, HARM], var_ref.at[row], out_sem.at[0, 1], out_sem.at[1, 1], to)

        @pl.when(half == core)
        def _():
            for k in range(HARM):
                coef_ref[k, row] = out[i, k]
            var_ref[row] = out[i, HARM]

    def step(flow, stage, i):
        if stage == 0:
            begin(flow, i)
        elif stage == 1:
            second(flow, i)
        elif stage == 2:
            reduce_raw(flow, i)
        elif stage == 5:
            finish(flow, i)
        else:
            exchange(flow, i, stage - 2)

    order = sorted((KEY[f][s], f, s) for f in range(len(FLOWS)) for s in range(STAGES))

    @pl.loop(0, max(u + max(d) for u, d in zip(UNITS, DELAY)))
    def _(turn):
        @pl.when(turn == min(d[2] for d in DELAY))
        def _():
            table_copy.wait()

        for _, number, stage in order:
            flow = flows[number]
            unit = turn - DELAY[number][stage]

            @pl.when((unit >= 0) & (unit < flow["units"]))
            def _(flow=flow, stage=stage, unit=unit):
                step(flow, stage, unit)

    every = x_ref.reshape(3 * 16 * 64, 8, 128)
    counts = [32 * 48, 32 * 16, 32 * 48]
    for stage in range(3):
        counts.append(sum(u * (4 >> stage) * f["rows"][stage][1] for u, f in zip(UNITS, flows)))
    for kind, count in enumerate(counts):
        await_bytes(every.at[pl.ds(0, count)], send.at[kind])
    for k in range(2):
        await_bytes(coef_ref.at[:, 0:16], out_sem.at[k, 0])
        await_bytes(var_ref.at[0:16], out_sem.at[k, 1])


def store(coef_vmem, var_vmem, coef_ref, var_ref, sems):
    copies = [pltpu.make_async_copy(coef_vmem.at[k], coef_ref.at[k], sems.at[k]) for k in range(HARM)]
    copies.append(pltpu.make_async_copy(var_vmem, var_ref, sems.at[HARM]))
    for copy in copies:
        copy.start()
    for copy in copies:
        copy.wait()


def local(snapshots):
    table, fit, root = constants()
    tiles = snapshots.reshape(48, 8, 64, 128).transpose(0, 2, 1, 3)
    tiles = tiles.reshape(3, 16, 4, 4, 2, 2, 8, 128)
    coeffs, variance = pl.pallas_call(
        functools.partial(kernel, fit, root),
        out_shape=(
            pltpu.VMEM((HARM, 32, 8, 128), jnp.float32),
            pltpu.VMEM((32, 8, 128), jnp.float32),
        ),
        in_specs=[pl.BlockSpec(memory_space=pl.ANY), pl.BlockSpec(memory_space=pl.ANY)],
        out_specs=(pl.BlockSpec(memory_space=pltpu.VMEM), pl.BlockSpec(memory_space=pltpu.VMEM)),
        scratch_shapes=scratch(),
        compiler_params=pltpu.CompilerParams(
            collective_id=0, has_side_effects=True, vmem_limit_bytes=VMEM_LIMIT
        ),
    )(jnp.asarray(table.reshape(-1), dtype=jnp.float32), tiles)
    coeffs, variance = pl.pallas_call(
        store,
        out_shape=(
            jax.ShapeDtypeStruct((HARM, 32, 8, 128), jnp.float32),
            jax.ShapeDtypeStruct((32, 8, 128), jnp.float32),
        ),
        in_specs=[pl.BlockSpec(memory_space=pltpu.VMEM)] * 2,
        out_specs=(pl.BlockSpec(memory_space=pl.ANY), pl.BlockSpec(memory_space=pl.ANY)),
        scratch_shapes=[pltpu.SemaphoreType.DMA((HARM + 1,))],
        compiler_params=pltpu.CompilerParams(vmem_limit_bytes=4 * 1024 * 1024),
    )(coeffs, variance)
    return coeffs.reshape(HARM, 256, 128), variance.reshape(256, 128)


def solution(mesh):
    return jax.shard_map(
        local,
        mesh=mesh,
        in_specs=(P(("rep", "io"), None),),
        out_specs=(P("rep", None, "io"), P("rep", "io")),
        check_vma=False,
    )
```

```python
import functools

import jax
import jax.numpy as jnp
import numpy as np
from jax import lax
from jax.experimental import pallas as pl
from jax.experimental.pallas import tpu as pltpu
from jax.sharding import PartitionSpec as P

TIMES = 96
HARM = 16
MONTHS = 12
EXTRA = 4
STAGES = 6
VMEM_LIMIT = 60817408
FLOWS = (
    ("zz", 1, "xxy", 1),
    ("zz", 3, "xxy", 3),
    ("zz", 1, "yxx", 1),
    ("zz", 3, "yxx", 3),
    ("xx", 1, "yzz", 1),
    ("xx", 3, "yzz", 3),
)
UNITS = (6, 6, 2, 2, 8, 8)
DELAY = (
    (1, 5, 8, 10, 13, 16),
    (0, 5, 7, 10, 13, 15),
    (0, 2, 4, 12, 16, 20),
    (4, 6, 8, 12, 15, 19),
    (0, 3, 5, 7, 10, 14),
    (0, 3, 4, 7, 10, 13),
)
POOL = (8, 2, 8, 6, 6, 2, 8, 8, 2, 2, 8, 8, 6, 6, 2)
SEMS = (
    (4, 13, 3, 4, 11),
    (3, 12, 2, 12, 13),
    (1, 5, 9, 8, 14),
    (8, 14, 1, 5, 1),
    (0, 6, 11, 7, 6),
    (2, 7, 10, 0, 10),
)
KEY = (
    (10, 25, 17, 14, 21, 16),
    (20, 24, 28, 30, 0, 22),
    (7, 18, 13, 35, 4, 12),
    (9, 26, 32, 19, 31, 8),
    (3, 1, 5, 34, 23, 15),
    (11, 2, 27, 6, 29, 33),
)


def constants():
    steps = np.arange(TIMES, dtype=np.float64)
    columns = [np.ones_like(steps), (steps - (TIMES - 1) / 2.0) / (TIMES / 2.0)]
    for harmonic in range(1, 7):
        columns.append(np.cos(2.0 * np.pi * harmonic * steps / 12.0))
    for harmonic in range(1, 6):
        columns.append(np.sin(2.0 * np.pi * harmonic * steps / 12.0))
    columns.append(np.cos(2.0 * np.pi * steps / TIMES))
    columns.append(np.sin(2.0 * np.pi * steps / TIMES))
    columns.append(np.cos(4.0 * np.pi * steps / TIMES))
    basis = np.stack(columns, axis=1)
    others = (1, 13, 14, 15)
    gather = np.zeros((HARM, MONTHS + EXTRA))
    for row in range(HARM):
        if row in others:
            gather[row, MONTHS + others.index(row)] = 1.0
        else:
            gather[row, :MONTHS] = basis[:MONTHS, row]
    gram = basis.T @ basis
    fit = np.linalg.solve(gram, gather)
    root = np.linalg.cholesky(gather.T @ fit)
    table = basis[:, others]
    return table, fit, root


def flip(v, mask):
    if mask == 1:
        return v + 1 - 2 * lax.rem(v, 2)
    if mask == 3:
        return 3 - v
    return lax.rem(v + 2, 4)

def plan(flow):
    raw, _, post, _ = flow
    merged = {"zz": set(), "xx": {"x"}, "yxx": {"x", "y"}}[raw]
    values = {"zz": 8, "xx": 11, "yxx": 17}[raw]
    rows = []
    for axis in post:
        joins = axis in ("x", "y") and axis not in merged
        after = values
        if joins:
            after = values + (3 if not merged else 6)
        rows.append((axis, values, after, tuple(sorted(merged)), joins))
        if joins:
            merged.add(axis)
        values = after
    return rows


def flow_shapes(number):
    units = UNITS[number]
    rows = plan(FLOWS[number])
    if FLOWS[number][0] == "yxx":
        dims = {"r1": (2, 3, 4, 4), "r2": (2, 2, 3, 4), "r3": (2, 2, 3, 4)}
    else:
        dims = {"r1": (2, 2, 3, 4, 2), "r2": (2, 3, 4, 2)}
    blocks = (2,) * len(rows)
    dims["s0"] = blocks + (rows[0][1],)
    for at, (_, before, after, _, joins) in enumerate(rows):
        blocks = blocks[1:]
        dims[f"r{at + 6 - len(rows)}"] = blocks + (before,)
        if joins:
            dims[f"s{at + 1}"] = blocks + (after,)
    dims["out"] = (HARM + 1,)
    return {name: (units,) + dim + (8, 128) for name, dim in dims.items()}


def sent_tiles(number):
    rows = plan(FLOWS[number])
    return [48] * (5 - len(rows)) + [before << (len(rows) - 1 - at) for at, (_, before, *_) in enumerate(rows)]


def scratch():
    shapes = []
    for number in range(len(FLOWS)):
        for shape in flow_shapes(number).values():
            shapes.append(pltpu.VMEM(shape, jnp.float32))
    for units in POOL:
        shapes.append(pltpu.SemaphoreType.DMA((units,)))
    shapes.append(pltpu.SemaphoreType.DMA((STAGES,)))
    shapes.append(pltpu.SMEM((TIMES * EXTRA,), jnp.float32))
    shapes.append(pltpu.SemaphoreType.DMA(()))
    shapes.append(pltpu.SemaphoreType.DMA((2, 2)))
    return shapes


def kernel(fit, root, table_hbm, x_ref, coef_ref, var_ref, *refs):
    me = lax.axis_index("io")
    core = lax.rem(me, 2)
    y = lax.rem(lax.div(me, 2), 2)
    x = lax.rem(lax.div(me, 4), 4)
    z = lax.div(me, 16)
    parity = lax.rem(x, 2)

    def dev(zz, xx, yy, cc):
        return ((zz * 4 + xx) * 2 + yy) * 2 + cc

    refs = list(refs)
    out_sem = refs.pop()
    table_sem = refs.pop()
    table_ref = refs.pop()
    send = refs.pop()
    table_copy = pltpu.make_async_copy(table_hbm, table_ref, table_sem)
    table_copy.start()
    flows = []
    at, base = 0, 0
    for number, spec in enumerate(FLOWS):
        raw, first, post, ring = spec
        flow = {"raw": raw, "f": first, "g": 4 - first, "post": post, "pf": ring, "pg": 4 - ring}
        flow["base"], flow["units"], flow["rows"] = base, UNITS[number], plan(spec)
        base += UNITS[number]
        for name in flow_shapes(number):
            flow[name] = refs[at]
            at += 1
        flow["swap"] = flow["base"] % 2 == 0 and UNITS[number] % 2 == 0
        flows.append(flow)
    for flow, pool in zip(flows, SEMS):
        flow["sem"] = {f"r{k + 1}": refs[at + pool[k]] for k in range(5)}

    def push(src, dst, send, recv, device):
        pltpu.make_async_remote_copy(
            src_ref=src,
            dst_ref=dst,
            send_sem=send,
            recv_sem=recv,
            device_id={"io": device},
            device_id_type=pl.DeviceIdType.MESH,
        ).start()

    def await_bytes(ref, sem):
        pltpu.make_async_copy(ref, ref, sem).wait()

    barrier = pltpu.get_barrier_semaphore()
    friends = [dev(z, x, y, 1 - core), dev(z, x, 1 - y, core)]
    for mask in (1, 3):
        for c in (core, 1 - core):
            friends.append(dev(flip(z, mask), x, y, c))
            friends.append(dev(z, flip(x, mask), y, c))
    for friend in friends:
        pl.semaphore_signal(barrier, inc=1, device_id={"io": friend}, device_id_type=pl.DeviceIdType.MESH)
    pl.semaphore_wait(barrier, len(friends))

    def place(flow, i, c):
        unit = flow["base"] + i
        half = lax.rem(i + 1 + c, 2) if flow["swap"] else lax.rem(unit, 2)
        return lax.div(unit, 2), half

    def begin_y(flow, i):
        lat, half = place(flow, i, core)
        _, half_other = place(flow, i, 1 - core)
        for home, yy in ((1, 1 - y), (0, y)):
            for group, when in ((0, core), (2, core + 1), (1, 2 * core)):
                src = x_ref.at[group, lat, :, :, yy, half_other if group == 1 else half]
                dst = flow["r1"].at[i, home, when]
                recv = flow["sem"]["r1"].at[i]
                c = 1 - core if group == 1 else core
                if home:
                    push(src, dst, send.at[0], recv, dev(z, x, yy, c))
                elif group == 1:
                    push(src, dst, send.at[1], recv, dev(z, x, yy, c))
                else:
                    pltpu.make_async_copy(src, dst, recv).start()

    def second_y(flow, i):
        await_bytes(flow["r1"].at[i], flow["sem"]["r1"].at[i])
        to = flip(x, flow["f"])
        for slot, block in ((1, flip(x, 2)), (0, to)):
            push(flow["r1"].at[i, :, :, :, block], flow["r2"].at[i, slot], send.at[2], flow["sem"]["r2"].at[i], dev(z, to, y, core))

    def third_y(flow, i):
        await_bytes(flow["r2"].at[i], flow["sem"]["r2"].at[i])
        to = flip(x, flow["g"])
        device = dev(z, to, y, core)
        push(flow["r1"].at[i, :, :, :, to], flow["r3"].at[i, 0], send.at[3], flow["sem"]["r3"].at[i], device)
        push(flow["r2"].at[i, 1], flow["r3"].at[i, 1], send.at[3], flow["sem"]["r3"].at[i], device)

    def begin(flow, i):
        lat, half = place(flow, i, core)
        _, half_other = place(flow, i, 1 - core)
        sem = flow["sem"]
        along_z = flow["raw"] == "zz"
        here = z if along_z else x
        there = flip(here, flow["f"])
        for at_home in (False, True):
            spot = here if at_home else there
            zz, xx = (spot, x) if along_z else (z, spot)
            for slot, block in ((0, spot), (1, flip(spot, flow["g"]))):
                for group, when in ((0, core), (2, core + 1), (1, 2 * core)):
                    lon = half_other if group == 1 else half
                    if along_z:
                        src = x_ref.at[group, lat, block, :, :, lon]
                    else:
                        src = x_ref.at[group, lat, :, block, :, lon]
                    c = 1 - core if group == 1 else core
                    if not at_home:
                        push(src, flow["r1"].at[i, 1, slot, when], send.at[0], sem["r1"].at[i], dev(zz, xx, y, c))
                    elif group == 1:
                        push(src, flow["r1"].at[i, 0, slot, when], send.at[1], sem["r1"].at[i], dev(zz, xx, y, c))
                    else:
                        pltpu.make_async_copy(src, flow["r1"].at[i, 0, slot, when], sem["r1"].at[i]).start()

    def second(flow, i):
        sem = flow["sem"]
        await_bytes(flow["r1"].at[i], sem["r1"].at[i])
        if flow["raw"] == "zz":
            to = dev(flip(z, flow["g"]), x, y, core)
        else:
            to = dev(z, flip(x, flow["g"]), y, core)
        push(flow["r1"].at[i, 0, 1], flow["r2"].at[i, 0], send.at[2], sem["r2"].at[i], to)
        push(flow["r1"].at[i, 1, 1], flow["r2"].at[i, 1], send.at[2], sem["r2"].at[i], to)

    def partner(flow, stage):
        axis = flow["post"][stage]
        if axis == "y":
            return dev(z, x, 1 - y, core)
        mask = flow["pg"] if axis in flow["post"][:stage] else flow["pf"]
        if axis == "x":
            return dev(z, flip(x, mask), y, core)
        return dev(flip(z, mask), x, y, core)

    def send_stats(flow, i, stage, state):
        step = stage + 6 - len(flow["rows"])
        name = f"r{step}"
        push(state.at[1], flow[name].at[i], send.at[step], flow["sem"][name].at[i], partner(flow, stage))

    def weights(chip, k):
        base = (chip * 3 + k) * EXTRA
        return [table_ref[base + j] for j in range(EXTRA)]

    def fold(pieces):
        sums, moments, total = {}, [None] * EXTRA, None
        for kind, k, value, chip in pieces:
            key = (kind, k)
            sums[key] = value if key not in sums else sums[key] + value
            w = weights(chip, k)
            for j in range(EXTRA):
                term = w[j] * value
                moments[j] = term if moments[j] is None else moments[j] + term
            square = value * value
            total = square if total is None else total + square
        return sums, moments, total

    def reduce_y(flow, i):
        await_bytes(flow["r3"].at[i], flow["sem"]["r3"].at[i])
        r1, r2, r3, s0 = flow["r1"], flow["r2"], flow["r3"], flow["s0"]
        spots = (x, flip(x, flow["f"]), flip(x, flow["g"]), flip(x, 2))
        for b0 in (1, 0):
            for b1 in range(2):
                lon = (b0 * flow["pf"]) ^ (b1 * flow["pg"])
                block = z if lon == 0 else flip(z, lon)
                pieces = []
                for k in range(3):
                    for b, yy in enumerate((y, 1 - y)):
                        values = (r1[i, b, k, block, x], r2[i, 0, b, k, block], r3[i, 0, b, k, block], r3[i, 1, b, k, block])
                        for number, value in enumerate(values):
                            a = 0 if number in (0, 3) else 1
                            pieces.append(((a, b), k, value, z * 8 + spots[number] * 2 + yy))
                sums, moments, total = fold(pieces)
                for ((a, b), k), value in sums.items():
                    xl = 1 - parity if a else parity
                    yy = 1 - y if b else y
                    s0[i, b0, b1, 3 * (2 * xl + yy) + k] = value
                for j in range(EXTRA):
                    s0[i, b0, b1, MONTHS + j] = moments[j]
                s0[i, b0, b1, MONTHS + EXTRA] = total
        send_stats(flow, i, 0, s0.at[i])

    def reduce_raw(flow, i):
        await_bytes(flow["r2"].at[i], flow["sem"]["r2"].at[i])
        r1, r2, s0 = flow["r1"], flow["r2"], flow["s0"]
        f, g, post = flow["f"], flow["g"], flow["post"]
        along_z = flow["raw"] == "zz"
        here = z if along_z else x
        spots = (here, flip(here, f), flip(here, g), flip(here, 2))
        chips = [spot * 8 + x * 2 + y if along_z else z * 8 + spot * 2 + y for spot in spots]
        across = x if along_z else z
        ring = "x" if along_z else "z"
        for b0 in (1, 0):
            for b1 in range(2):
                for b2 in range(2):
                    bits = (b0, b1, b2)
                    lon, lon_y, seen = 0, y, False
                    for bit, axis in zip(bits, post):
                        if axis == "y":
                            lon_y = 1 - y if bit else y
                        else:
                            lon = lon ^ (bit * (flow["pg"] if seen else flow["pf"]))
                            seen = True
                    block = across if lon == 0 else flip(across, lon)
                    pieces = []
                    for k in range(3):
                        values = (
                            r1[i, 0, 0, k, block, lon_y],
                            r1[i, 1, 0, k, block, lon_y],
                            r2[i, 0, k, block, lon_y],
                            r2[i, 1, k, block, lon_y],
                        )
                        for number, value in enumerate(values):
                            kind = 0 if along_z or number in (0, 3) else 1
                            pieces.append((kind, k, value, chips[number]))
                    sums, moments, total = fold(pieces)
                    for (a, k), value in sums.items():
                        if along_z:
                            s0[i, b0, b1, b2, k] = value
                        else:
                            s0[i, b0, b1, b2, 3 * (1 - parity if a else parity) + k] = value
                    months = 3 if along_z else 6
                    for j in range(EXTRA):
                        s0[i, b0, b1, b2, months + j] = moments[j]
                    s0[i, b0, b1, b2, months + EXTRA] = total
        send_stats(flow, i, 0, s0.at[i])

    def merge(flow, i, stage):
        name = f"r{stage + 6 - len(flow['rows'])}"
        await_bytes(flow[name].at[i], flow["sem"][name].at[i])
        axis, before, after, merged, joins = flow["rows"][stage]
        theirs = flow[name].at[i]
        mine = flow["state"].at[0]
        blocks = [()]
        for _ in range(len(flow["rows"]) - 1 - stage):
            blocks = [b + (bit,) for b in blocks for bit in (1, 0)]
        if not joins:
            for b in blocks:
                mine[b] = mine[b] + theirs[b]
            return mine
        new = flow[f"s{stage + 1}"].at[i]
        own_class = parity if axis == "x" else y
        months = before - EXTRA - 1
        for b in blocks:
            for k in range(months):
                if not merged:
                    spot = [3 * c + k for c in (own_class, 1 - own_class)]
                elif axis == "y":
                    spot = [6 * (k // 3) + 3 * c + k % 3 for c in (own_class, 1 - own_class)]
                else:
                    spot = [6 * c + k for c in (own_class, 1 - own_class)]
                new[b + (spot[0],)] = mine[b + (k,)]
                new[b + (spot[1],)] = theirs[b + (k,)]
            for j in range(EXTRA + 1):
                new[b + (2 * months + j,)] = mine[b + (months + j,)] + theirs[b + (months + j,)]
        return new

    def exchange(flow, i, stage):
        flow["state"] = flow["s0"].at[i]
        for done in range(stage - 1):
            joins = flow["rows"][done][4]
            flow["state"] = flow[f"s{done + 1}"].at[i] if joins else flow["state"].at[0]
        state = merge(flow, i, stage - 1)
        if stage < len(flow["rows"]):
            send_stats(flow, i, stage, state)
        return state

    def finish(flow, i):
        state = exchange(flow, i, len(flow["rows"]))
        out = flow["out"]
        w = [state[j] for j in range(MONTHS + EXTRA)]
        total = state[MONTHS + EXTRA]
        for row in range(HARM):
            value = None
            for j in range(MONTHS + EXTRA):
                term = w[j] * float(np.float32(fit[row, j]))
                value = term if value is None else value + term
            out[i, row] = value
        explained = None
        for col in range(HARM):
            value = None
            for j in range(col, HARM):
                if abs(root[j, col]) < 1e-12:
                    continue
                term = w[j] * float(np.float32(root[j, col]))
                value = term if value is None else value + term
            explained = value * value if explained is None else explained + value * value
        out[i, HARM] = (total - explained) * (1.0 / TIMES)
        lat, half = place(flow, i, core)
        row = core * 16 + lat

        @pl.when(half != core)
        def _():
            to = dev(z, x, y, 1 - core)
            push(out.at[i, 0:HARM], coef_ref.at[:, row], out_sem.at[0, 0], out_sem.at[1, 0], to)
            push(out.at[i, HARM], var_ref.at[row], out_sem.at[0, 1], out_sem.at[1, 1], to)

        @pl.when(half == core)
        def _():
            for k in range(HARM):
                coef_ref[k, row] = out[i, k]
            var_ref[row] = out[i, HARM]

    def step(flow, stage, i):
        early = (begin, second, reduce_raw)
        if flow["raw"] == "yxx":
            early = (begin_y, second_y, third_y, reduce_y)
        if stage < len(early):
            early[stage](flow, i)
        elif stage == 5:
            finish(flow, i)
        else:
            exchange(flow, i, stage + 1 - len(early))

    order = sorted((KEY[f][s], f, s) for f in range(len(FLOWS)) for s in range(STAGES))

    @pl.loop(0, max(u + max(d) for u, d in zip(UNITS, DELAY)))
    def _(turn):
        @pl.when(turn == min(d[5 - len(f["rows"])] for d, f in zip(DELAY, flows)))
        def _():
            table_copy.wait()

        for _, number, stage in order:
            flow = flows[number]
            unit = turn - DELAY[number][stage]

            @pl.when((unit >= 0) & (unit < flow["units"]))
            def _(flow=flow, stage=stage, unit=unit):
                step(flow, stage, unit)

    every = x_ref.reshape(3 * 16 * 64, 8, 128)
    totals = [sum(u * sent_tiles(n)[k] for n, u in enumerate(UNITS)) for k in range(5)]
    counts = [totals[0], 32 * 16] + totals[1:]
    for kind, count in enumerate(counts):
        await_bytes(every.at[pl.ds(0, count)], send.at[kind])
    for k in range(2):
        await_bytes(coef_ref.at[:, 0:16], out_sem.at[k, 0])
        await_bytes(var_ref.at[0:16], out_sem.at[k, 1])


def store(coef_vmem, var_vmem, coef_ref, var_ref, sems):
    copies = [pltpu.make_async_copy(coef_vmem.at[k], coef_ref.at[k], sems.at[k]) for k in range(HARM)]
    copies.append(pltpu.make_async_copy(var_vmem, var_ref, sems.at[HARM]))
    for copy in copies:
        copy.start()
    for copy in copies:
        copy.wait()


def local(snapshots):
    table, fit, root = constants()
    tiles = snapshots.reshape(48, 8, 64, 128).transpose(0, 2, 1, 3)
    tiles = tiles.reshape(3, 16, 4, 4, 2, 2, 8, 128)
    coeffs, variance = pl.pallas_call(
        functools.partial(kernel, fit, root),
        out_shape=(
            pltpu.VMEM((HARM, 32, 8, 128), jnp.float32),
            pltpu.VMEM((32, 8, 128), jnp.float32),
        ),
        in_specs=[pl.BlockSpec(memory_space=pl.ANY), pl.BlockSpec(memory_space=pl.ANY)],
        out_specs=(pl.BlockSpec(memory_space=pltpu.VMEM), pl.BlockSpec(memory_space=pltpu.VMEM)),
        scratch_shapes=scratch(),
        compiler_params=pltpu.CompilerParams(
            collective_id=0, has_side_effects=True, vmem_limit_bytes=VMEM_LIMIT
        ),
    )(jnp.asarray(table.reshape(-1), dtype=jnp.float32), tiles)
    coeffs, variance = pl.pallas_call(
        store,
        out_shape=(
            jax.ShapeDtypeStruct((HARM, 32, 8, 128), jnp.float32),
            jax.ShapeDtypeStruct((32, 8, 128), jnp.float32),
        ),
        in_specs=[pl.BlockSpec(memory_space=pltpu.VMEM)] * 2,
        out_specs=(pl.BlockSpec(memory_space=pl.ANY), pl.BlockSpec(memory_space=pl.ANY)),
        scratch_shapes=[pltpu.SemaphoreType.DMA((HARM + 1,))],
        compiler_params=pltpu.CompilerParams(vmem_limit_bytes=4 * 1024 * 1024),
    )(coeffs, variance)
    return coeffs.reshape(HARM, 256, 128), variance.reshape(256, 128)


def solution(mesh):
    return jax.shard_map(
        local,
        mesh=mesh,
        in_specs=(P(("rep", "io"), None),),
        out_specs=(P("rep", None, "io"), P("rep", "io")),
        check_vma=False,
    )
```

```python
import functools

import jax
import jax.numpy as jnp
import numpy as np
from jax import lax
from jax.experimental import pallas as pl
from jax.experimental.pallas import tpu as pltpu
from jax.sharding import PartitionSpec as P

TIMES = 96
HARM = 16
MONTHS = 12
EXTRA = 4
STAGES = 6
VMEM_LIMIT = 60817408
FLOWS = (
    ("zz", 3, "xyx", 3),
    ("zz", 1, "xyx", 1),
    ("xx", 1, "zzy", 1),
    ("xx", 3, "zzy", 3),
    ("xx", 1, "yzz", 1),
    ("xx", 3, "yzz", 3),
    ("zz", 1, "yxx", 1),
    ("zz", 3, "yxx", 3),
    ("yxx", 1, "zz", 1),
    ("yxx", 3, "zz", 3),
)
UNITS = (2, 2, 2, 2, 4, 4, 5, 5, 3, 3)
DELAY = (
    (4, 7, 9, 14, 17, 20),
    (3, 7, 10, 13, 16, 20),
    (3, 7, 9, 10, 16, 19),
    (0, 5, 7, 10, 12, 15),
    (0, 4, 5, 7, 14, 18),
    (2, 4, 5, 8, 14, 18),
    (0, 3, 6, 9, 13, 17),
    (0, 4, 6, 10, 13, 17),
    (1, 7, 9, 11, 15, 19),
    (1, 6, 7, 9, 14, 18),
)
POOL = (5, 5, 5, 5, 5, 5, 4, 4, 4, 4, 4, 4, 3, 3, 2, 2, 2, 2, 2, 2, 2, 2, 2, 2)
SEMS = (
    ((17, 2), (20, 2), (16, 2), (23, 2), (12, 2)),
    ((15, 2), (22, 2), (12, 2), (15, 2), (14, 2)),
    ((16, 2), (19, 2), (14, 2), (18, 2), (21, 2)),
    ((14, 2), (18, 2), (21, 2), (17, 2), (19, 2)),
    ((6, 4), (8, 4), (10, 4), (1, 4), (9, 4)),
    ((7, 4), (9, 4), (11, 4), (6, 4), (7, 4)),
    ((1, 5), (2, 5), (4, 5), (2, 5), (0, 5)),
    ((0, 5), (3, 5), (5, 5), (3, 5), (4, 5)),
    ((12, 3), (7, 3), (13, 3), (10, 3), (11, 3)),
    ((13, 3), (0, 3), (9, 3), (8, 3), (5, 3)),
)
KEY = (
    (25, 44, 55, 12, 14, 9),
    (38, 56, 19, 17, 34, 40),
    (50, 29, 16, 30, 27, 7),
    (10, 45, 52, 15, 47, 20),
    (58, 11, 36, 23, 57, 43),
    (21, 22, 42, 49, 3, 13),
    (51, 24, 18, 46, 28, 8),
    (1, 0, 41, 26, 54, 4),
    (31, 32, 5, 33, 35, 6),
    (37, 2, 59, 48, 39, 53),
)


def constants():
    steps = np.arange(TIMES, dtype=np.float64)
    columns = [np.ones_like(steps), (steps - (TIMES - 1) / 2.0) / (TIMES / 2.0)]
    for harmonic in range(1, 7):
        columns.append(np.cos(2.0 * np.pi * harmonic * steps / 12.0))
    for harmonic in range(1, 6):
        columns.append(np.sin(2.0 * np.pi * harmonic * steps / 12.0))
    columns.append(np.cos(2.0 * np.pi * steps / TIMES))
    columns.append(np.sin(2.0 * np.pi * steps / TIMES))
    columns.append(np.cos(4.0 * np.pi * steps / TIMES))
    basis = np.stack(columns, axis=1)
    others = (1, 13, 14, 15)
    gather = np.zeros((HARM, MONTHS + EXTRA))
    for row in range(HARM):
        if row in others:
            gather[row, MONTHS + others.index(row)] = 1.0
        else:
            gather[row, :MONTHS] = basis[:MONTHS, row]
    gram = basis.T @ basis
    fit = np.linalg.solve(gram, gather)
    root = np.linalg.cholesky(gather.T @ fit)
    table = basis[:, others]
    return table, fit, root


def flip(v, mask):
    if mask == 1:
        return v + 1 - 2 * lax.rem(v, 2)
    if mask == 3:
        return 3 - v
    return lax.rem(v + 2, 4)

def plan(flow):
    raw, _, post, _ = flow
    merged = {"zz": set(), "xx": {"x"}, "yxx": {"x", "y"}}[raw]
    values = {"zz": 8, "xx": 11, "yxx": 17}[raw]
    rows = []
    for axis in post:
        joins = axis in ("x", "y") and axis not in merged
        after = values
        if joins:
            after = values + (3 if not merged else 6)
        rows.append((axis, values, after, tuple(sorted(merged)), joins))
        if joins:
            merged.add(axis)
        values = after
    return rows


def flow_shapes(number):
    units = UNITS[number]
    rows = plan(FLOWS[number])
    if FLOWS[number][0] == "yxx":
        dims = {"r1": (2, 3, 4, 4), "r2": (2, 2, 3, 4), "r3": (2, 2, 3, 4)}
    else:
        dims = {"r1": (2, 2, 3, 4, 2), "r2": (2, 3, 4, 2)}
    blocks = (2,) * len(rows)
    dims["s0"] = blocks + (rows[0][1],)
    for at, (_, before, after, _, joins) in enumerate(rows):
        blocks = blocks[1:]
        dims[f"r{at + 6 - len(rows)}"] = blocks + (before,)
        if joins:
            dims[f"s{at + 1}"] = blocks + (after,)
    dims["out"] = (HARM + 1,)
    return {name: (units,) + dim + (8, 128) for name, dim in dims.items()}


def sent_tiles(number):
    rows = plan(FLOWS[number])
    return [48] * (5 - len(rows)) + [before << (len(rows) - 1 - at) for at, (_, before, *_) in enumerate(rows)]


def scratch():
    shapes = []
    for number in range(len(FLOWS)):
        for shape in flow_shapes(number).values():
            shapes.append(pltpu.VMEM(shape, jnp.float32))
    for units in POOL:
        shapes.append(pltpu.SemaphoreType.DMA((units,)))
    shapes.append(pltpu.SemaphoreType.DMA((STAGES,)))
    shapes.append(pltpu.SMEM((TIMES * EXTRA,), jnp.float32))
    shapes.append(pltpu.SemaphoreType.DMA(()))
    shapes.append(pltpu.SemaphoreType.DMA((2, 2)))
    return shapes


def kernel(fit, root, table_hbm, x_ref, coef_ref, var_ref, *refs):
    me = lax.axis_index("io")
    core = lax.rem(me, 2)
    y = lax.rem(lax.div(me, 2), 2)
    x = lax.rem(lax.div(me, 4), 4)
    z = lax.div(me, 16)
    parity = lax.rem(x, 2)

    def dev(zz, xx, yy, cc):
        return ((zz * 4 + xx) * 2 + yy) * 2 + cc

    refs = list(refs)
    out_sem = refs.pop()
    table_sem = refs.pop()
    table_ref = refs.pop()
    send = refs.pop()
    table_copy = pltpu.make_async_copy(table_hbm, table_ref, table_sem)
    table_copy.start()
    flows = []
    at, base = 0, 0
    for number, spec in enumerate(FLOWS):
        raw, first, post, ring = spec
        flow = {"raw": raw, "f": first, "g": 4 - first, "post": post, "pf": ring, "pg": 4 - ring}
        flow["base"], flow["units"], flow["rows"] = base, UNITS[number], plan(spec)
        base += UNITS[number]
        for name in flow_shapes(number):
            flow[name] = refs[at]
            at += 1
        flow["swap"] = flow["base"] % 2 == 0 and UNITS[number] % 2 == 0
        flows.append(flow)
    for flow, pool in zip(flows, SEMS):
        flow["sem"] = {f"r{k + 1}": (refs[at + pool[k][0]], pool[k][1]) for k in range(5)}

    def arrival(flow, name, i):
        ref, length = flow["sem"][name]
        return ref.at[i if length == flow["units"] else lax.rem(i, length)]

    def push(src, dst, send, recv, device):
        pltpu.make_async_remote_copy(
            src_ref=src,
            dst_ref=dst,
            send_sem=send,
            recv_sem=recv,
            device_id={"io": device},
            device_id_type=pl.DeviceIdType.MESH,
        ).start()

    def await_bytes(ref, sem):
        pltpu.make_async_copy(ref, ref, sem).wait()

    barrier = pltpu.get_barrier_semaphore()
    friends = [dev(z, x, y, 1 - core), dev(z, x, 1 - y, core), dev(z, x, 1 - y, 1 - core)]
    for mask in (1, 3):
        for c in (core, 1 - core):
            friends.append(dev(flip(z, mask), x, y, c))
            friends.append(dev(z, flip(x, mask), y, c))
    for friend in friends:
        pl.semaphore_signal(barrier, inc=1, device_id={"io": friend}, device_id_type=pl.DeviceIdType.MESH)
    pl.semaphore_wait(barrier, len(friends))

    def place(flow, i, c):
        unit = flow["base"] + i
        half = lax.rem(i + 1 + c, 2) if flow["swap"] else lax.rem(unit, 2)
        return lax.div(unit, 2), half

    def begin_y(flow, i):
        lat, half = place(flow, i, core)
        _, half_other = place(flow, i, 1 - core)
        for home, yy in ((1, 1 - y), (0, y)):
            for group, when in ((0, core), (2, core + 1), (1, 2 * core)):
                src = x_ref.at[group, lat, :, :, yy, half_other if group == 1 else half]
                dst = flow["r1"].at[i, home, when]
                recv = arrival(flow, "r1", i)
                c = 1 - core if group == 1 else core
                if home:
                    push(src, dst, send.at[0], recv, dev(z, x, yy, c))
                elif group == 1:
                    push(src, dst, send.at[1], recv, dev(z, x, yy, c))
                else:
                    pltpu.make_async_copy(src, dst, recv).start()

    def second_y(flow, i):
        await_bytes(flow["r1"].at[i], arrival(flow, "r1", i))
        to = flip(x, flow["f"])
        for slot, block in ((1, flip(x, 2)), (0, to)):
            push(flow["r1"].at[i, :, :, :, block], flow["r2"].at[i, slot], send.at[2], arrival(flow, "r2", i), dev(z, to, y, core))

    def third_y(flow, i):
        await_bytes(flow["r2"].at[i], arrival(flow, "r2", i))
        to = flip(x, flow["g"])
        device = dev(z, to, y, core)
        push(flow["r1"].at[i, :, :, :, to], flow["r3"].at[i, 0], send.at[3], arrival(flow, "r3", i), device)
        push(flow["r2"].at[i, 1], flow["r3"].at[i, 1], send.at[3], arrival(flow, "r3", i), device)

    def begin(flow, i):
        lat, half = place(flow, i, core)
        _, half_other = place(flow, i, 1 - core)
        along_z = flow["raw"] == "zz"
        here = z if along_z else x
        there = flip(here, flow["f"])
        for at_home in (False, True):
            spot = here if at_home else there
            zz, xx = (spot, x) if along_z else (z, spot)
            for slot, block in ((0, spot), (1, flip(spot, flow["g"]))):
                for group, when in ((0, core), (2, core + 1), (1, 2 * core)):
                    lon = half_other if group == 1 else half
                    if along_z:
                        src = x_ref.at[group, lat, block, :, :, lon]
                    else:
                        src = x_ref.at[group, lat, :, block, :, lon]
                    c = 1 - core if group == 1 else core
                    if not at_home:
                        push(src, flow["r1"].at[i, 1, slot, when], send.at[0], arrival(flow, "r1", i), dev(zz, xx, y, c))
                    elif group == 1:
                        push(src, flow["r1"].at[i, 0, slot, when], send.at[1], arrival(flow, "r1", i), dev(zz, xx, y, c))
                    else:
                        pltpu.make_async_copy(src, flow["r1"].at[i, 0, slot, when], arrival(flow, "r1", i)).start()

    def second(flow, i):
        await_bytes(flow["r1"].at[i], arrival(flow, "r1", i))
        if flow["raw"] == "zz":
            to = dev(flip(z, flow["g"]), x, y, core)
        else:
            to = dev(z, flip(x, flow["g"]), y, core)
        push(flow["r1"].at[i, 0, 1], flow["r2"].at[i, 0], send.at[2], arrival(flow, "r2", i), to)
        push(flow["r1"].at[i, 1, 1], flow["r2"].at[i, 1], send.at[2], arrival(flow, "r2", i), to)

    def partner(flow, stage):
        axis = flow["post"][stage]
        if axis == "y":
            return dev(z, x, 1 - y, core)
        mask = flow["pg"] if axis in flow["post"][:stage] else flow["pf"]
        if axis == "x":
            return dev(z, flip(x, mask), y, core)
        return dev(flip(z, mask), x, y, core)

    def send_stats(flow, i, stage, state):
        step = stage + 6 - len(flow["rows"])
        name = f"r{step}"
        push(state.at[1], flow[name].at[i], send.at[step], arrival(flow, name, i), partner(flow, stage))

    def weights(chip, k):
        base = (chip * 3 + k) * EXTRA
        return [table_ref[base + j] for j in range(EXTRA)]

    def fold(pieces):
        sums, moments, total = {}, [None] * EXTRA, None
        for kind, k, value, chip in pieces:
            key = (kind, k)
            sums[key] = value if key not in sums else sums[key] + value
            w = weights(chip, k)
            for j in range(EXTRA):
                term = w[j] * value
                moments[j] = term if moments[j] is None else moments[j] + term
            square = value * value
            total = square if total is None else total + square
        return sums, moments, total

    def reduce_y(flow, i):
        await_bytes(flow["r3"].at[i], arrival(flow, "r3", i))
        r1, r2, r3, s0 = flow["r1"], flow["r2"], flow["r3"], flow["s0"]
        spots = (x, flip(x, flow["f"]), flip(x, flow["g"]), flip(x, 2))
        for b0 in (1, 0):
            for b1 in range(2):
                lon = (b0 * flow["pf"]) ^ (b1 * flow["pg"])
                block = z if lon == 0 else flip(z, lon)
                pieces = []
                for k in range(3):
                    for b, yy in enumerate((y, 1 - y)):
                        values = (r1[i, b, k, block, x], r2[i, 0, b, k, block], r3[i, 0, b, k, block], r3[i, 1, b, k, block])
                        for number, value in enumerate(values):
                            a = 0 if number in (0, 3) else 1
                            pieces.append(((a, b), k, value, z * 8 + spots[number] * 2 + yy))
                sums, moments, total = fold(pieces)
                for ((a, b), k), value in sums.items():
                    xl = 1 - parity if a else parity
                    yy = 1 - y if b else y
                    s0[i, b0, b1, 3 * (2 * xl + yy) + k] = value
                for j in range(EXTRA):
                    s0[i, b0, b1, MONTHS + j] = moments[j]
                s0[i, b0, b1, MONTHS + EXTRA] = total
        send_stats(flow, i, 0, s0.at[i])

    def reduce_raw(flow, i):
        await_bytes(flow["r2"].at[i], arrival(flow, "r2", i))
        r1, r2, s0 = flow["r1"], flow["r2"], flow["s0"]
        f, g, post = flow["f"], flow["g"], flow["post"]
        along_z = flow["raw"] == "zz"
        here = z if along_z else x
        spots = (here, flip(here, f), flip(here, g), flip(here, 2))
        chips = [spot * 8 + x * 2 + y if along_z else z * 8 + spot * 2 + y for spot in spots]
        across = x if along_z else z
        ring = "x" if along_z else "z"
        for b0 in (1, 0):
            for b1 in range(2):
                for b2 in range(2):
                    bits = (b0, b1, b2)
                    lon, lon_y, seen = 0, y, False
                    for bit, axis in zip(bits, post):
                        if axis == "y":
                            lon_y = 1 - y if bit else y
                        else:
                            lon = lon ^ (bit * (flow["pg"] if seen else flow["pf"]))
                            seen = True
                    block = across if lon == 0 else flip(across, lon)
                    pieces = []
                    for k in range(3):
                        values = (
                            r1[i, 0, 0, k, block, lon_y],
                            r1[i, 1, 0, k, block, lon_y],
                            r2[i, 0, k, block, lon_y],
                            r2[i, 1, k, block, lon_y],
                        )
                        for number, value in enumerate(values):
                            kind = 0 if along_z or number in (0, 3) else 1
                            pieces.append((kind, k, value, chips[number]))
                    sums, moments, total = fold(pieces)
                    for (a, k), value in sums.items():
                        if along_z:
                            s0[i, b0, b1, b2, k] = value
                        else:
                            s0[i, b0, b1, b2, 3 * (1 - parity if a else parity) + k] = value
                    months = 3 if along_z else 6
                    for j in range(EXTRA):
                        s0[i, b0, b1, b2, months + j] = moments[j]
                    s0[i, b0, b1, b2, months + EXTRA] = total
        send_stats(flow, i, 0, s0.at[i])

    def merge(flow, i, stage):
        name = f"r{stage + 6 - len(flow['rows'])}"
        await_bytes(flow[name].at[i], arrival(flow, name, i))
        axis, before, after, merged, joins = flow["rows"][stage]
        theirs = flow[name].at[i]
        mine = flow["state"].at[0]
        blocks = [()]
        for _ in range(len(flow["rows"]) - 1 - stage):
            blocks = [b + (bit,) for b in blocks for bit in (1, 0)]
        if not joins:
            for b in blocks:
                mine[b] = mine[b] + theirs[b]
            return mine
        new = flow[f"s{stage + 1}"].at[i]
        own_class = parity if axis == "x" else y
        months = before - EXTRA - 1
        for b in blocks:
            for k in range(months):
                if not merged:
                    spot = [3 * c + k for c in (own_class, 1 - own_class)]
                elif axis == "y":
                    spot = [6 * (k // 3) + 3 * c + k % 3 for c in (own_class, 1 - own_class)]
                else:
                    spot = [6 * c + k for c in (own_class, 1 - own_class)]
                new[b + (spot[0],)] = mine[b + (k,)]
                new[b + (spot[1],)] = theirs[b + (k,)]
            for j in range(EXTRA + 1):
                new[b + (2 * months + j,)] = mine[b + (months + j,)] + theirs[b + (months + j,)]
        return new

    def exchange(flow, i, stage):
        flow["state"] = flow["s0"].at[i]
        for done in range(stage - 1):
            joins = flow["rows"][done][4]
            flow["state"] = flow[f"s{done + 1}"].at[i] if joins else flow["state"].at[0]
        state = merge(flow, i, stage - 1)
        if stage < len(flow["rows"]):
            send_stats(flow, i, stage, state)
        return state

    def finish(flow, i):
        state = exchange(flow, i, len(flow["rows"]))
        out = flow["out"]
        w = [state[j] for j in range(MONTHS + EXTRA)]
        total = state[MONTHS + EXTRA]
        for row in range(HARM):
            value = None
            for j in range(MONTHS + EXTRA):
                term = w[j] * float(np.float32(fit[row, j]))
                value = term if value is None else value + term
            out[i, row] = value
        explained = None
        for col in range(HARM):
            value = None
            for j in range(col, HARM):
                if abs(root[j, col]) < 1e-12:
                    continue
                term = w[j] * float(np.float32(root[j, col]))
                value = term if value is None else value + term
            explained = value * value if explained is None else explained + value * value
        out[i, HARM] = (total - explained) * (1.0 / TIMES)
        lat, half = place(flow, i, core)
        row = core * 16 + lat

        @pl.when(half != core)
        def _():
            to = dev(z, x, y, 1 - core)
            push(out.at[i, 0:HARM], coef_ref.at[:, row], out_sem.at[0, 0], out_sem.at[1, 0], to)
            push(out.at[i, HARM], var_ref.at[row], out_sem.at[0, 1], out_sem.at[1, 1], to)

        @pl.when(half == core)
        def _():
            for k in range(HARM):
                coef_ref[k, row] = out[i, k]
            var_ref[row] = out[i, HARM]

    def step(flow, stage, i):
        early = (begin, second, reduce_raw)
        if flow["raw"] == "yxx":
            early = (begin_y, second_y, third_y, reduce_y)
        if stage < len(early):
            early[stage](flow, i)
        elif stage == 5:
            finish(flow, i)
        else:
            exchange(flow, i, stage + 1 - len(early))

    order = sorted((KEY[f][s], f, s) for f in range(len(FLOWS)) for s in range(STAGES))

    @pl.loop(0, max(u + max(d) for u, d in zip(UNITS, DELAY)))
    def _(turn):
        @pl.when(turn == min(d[5 - len(f["rows"])] for d, f in zip(DELAY, flows)))
        def _():
            table_copy.wait()

        for _, number, stage in order:
            flow = flows[number]
            unit = turn - DELAY[number][stage]

            @pl.when((unit >= 0) & (unit < flow["units"]))
            def _(flow=flow, stage=stage, unit=unit):
                step(flow, stage, unit)

    every = x_ref.reshape(3 * 16 * 64, 8, 128)
    totals = [sum(u * sent_tiles(n)[k] for n, u in enumerate(UNITS)) for k in range(5)]
    counts = [totals[0], 32 * 16] + totals[1:]
    for kind, count in enumerate(counts):
        await_bytes(every.at[pl.ds(0, count)], send.at[kind])
    for k in range(2):
        await_bytes(coef_ref.at[:, 0:16], out_sem.at[k, 0])
        await_bytes(var_ref.at[0:16], out_sem.at[k, 1])


def store(coef_vmem, var_vmem, coef_ref, var_ref, sems):
    copies = [pltpu.make_async_copy(coef_vmem.at[k], coef_ref.at[k], sems.at[k]) for k in range(HARM)]
    copies.append(pltpu.make_async_copy(var_vmem, var_ref, sems.at[HARM]))
    for copy in copies:
        copy.start()
    for copy in copies:
        copy.wait()


def local(snapshots):
    table, fit, root = constants()
    tiles = snapshots.reshape(48, 8, 64, 128).transpose(0, 2, 1, 3)
    tiles = tiles.reshape(3, 16, 4, 4, 2, 2, 8, 128)
    coeffs, variance = pl.pallas_call(
        functools.partial(kernel, fit, root),
        out_shape=(
            pltpu.VMEM((HARM, 32, 8, 128), jnp.float32),
            pltpu.VMEM((32, 8, 128), jnp.float32),
        ),
        in_specs=[pl.BlockSpec(memory_space=pl.ANY), pl.BlockSpec(memory_space=pl.ANY)],
        out_specs=(pl.BlockSpec(memory_space=pltpu.VMEM), pl.BlockSpec(memory_space=pltpu.VMEM)),
        scratch_shapes=scratch(),
        compiler_params=pltpu.CompilerParams(
            collective_id=0, has_side_effects=True, vmem_limit_bytes=VMEM_LIMIT
        ),
    )(jnp.asarray(table.reshape(-1), dtype=jnp.float32), tiles)
    coeffs, variance = pl.pallas_call(
        store,
        out_shape=(
            jax.ShapeDtypeStruct((HARM, 32, 8, 128), jnp.float32),
            jax.ShapeDtypeStruct((32, 8, 128), jnp.float32),
        ),
        in_specs=[pl.BlockSpec(memory_space=pltpu.VMEM)] * 2,
        out_specs=(pl.BlockSpec(memory_space=pl.ANY), pl.BlockSpec(memory_space=pl.ANY)),
        scratch_shapes=[pltpu.SemaphoreType.DMA((HARM + 1,))],
        compiler_params=pltpu.CompilerParams(vmem_limit_bytes=4 * 1024 * 1024),
    )(coeffs, variance)
    return coeffs.reshape(HARM, 256, 128), variance.reshape(256, 128)


def solution(mesh):
    return jax.shard_map(
        local,
        mesh=mesh,
        in_specs=(P(("rep", "io"), None),),
        out_specs=(P("rep", None, "io"), P("rep", "io")),
        check_vma=False,
    )
```

```python
import functools

import jax
import jax.numpy as jnp
import numpy as np
from jax import lax
from jax.experimental import pallas as pl
from jax.experimental.pallas import tpu as pltpu
from jax.sharding import PartitionSpec as P

TIMES = 96
HARM = 16
MONTHS = 12
EXTRA = 4
STAGES = 6
VMEM_LIMIT = 60817408
FLOWS = (
    ("zz", 3, "xyx", 3),
    ("zz", 1, "xyx", 1),
    ("xx", 1, "zzy", 1),
    ("xx", 3, "zzy", 3),
    ("xx", 1, "yzz", 1),
    ("xx", 3, "yzz", 3),
    ("zz", 1, "yxx", 1),
    ("zz", 3, "yxx", 3),
    ("yxx", 1, "zz", 1),
    ("yxx", 3, "zz", 3),
)
UNITS = (2, 2, 2, 2, 4, 4, 5, 5, 3, 3)
DELAY = (
    (4, 7, 9, 14, 17, 20),
    (3, 7, 10, 13, 16, 20),
    (3, 7, 9, 10, 16, 19),
    (0, 5, 7, 10, 12, 15),
    (0, 4, 5, 7, 14, 18),
    (2, 4, 5, 8, 14, 18),
    (0, 3, 6, 9, 13, 17),
    (0, 4, 6, 10, 13, 17),
    (1, 7, 9, 11, 15, 19),
    (1, 6, 7, 9, 14, 18),
)
FIRST = (7, 3, 6, 4, 8)
POOL = (5, 5, 5, 5, 5, 5, 4, 4, 4, 4, 4, 4, 3, 3, 2, 2, 2, 2, 2, 2, 2, 2, 2, 2)
SEMS = (
    ((15, 2), (18, 2), (8, 2), (20, 2), (3, 2)),
    ((17, 2), (19, 2), (16, 2), (21, 2), (14, 2)),
    ((16, 2), (20, 2), (14, 2), (17, 2), (22, 2)),
    ((14, 2), (21, 2), (22, 2), (23, 2), (15, 2)),
    ((6, 4), (9, 4), (8, 4), (1, 4), (7, 4)),
    ((7, 4), (10, 4), (11, 4), (6, 4), (11, 4)),
    ((0, 5), (2, 5), (4, 5), (2, 5), (0, 5)),
    ((1, 5), (3, 5), (5, 5), (3, 5), (4, 5)),
    ((12, 3), (7, 3), (13, 3), (12, 3), (9, 3)),
    ((13, 3), (0, 3), (9, 3), (10, 3), (5, 3)),
)
KEY = (
    (25, 44, 55, 12, 14, 9),
    (38, 56, 19, 17, 34, 40),
    (50, 29, 16, 30, 27, 7),
    (10, 45, 52, 15, 47, 20),
    (58, 11, 36, 23, 57, 43),
    (21, 22, 42, 49, 3, 13),
    (51, 24, 18, 46, 28, 8),
    (1, 0, 41, 26, 54, 4),
    (31, 32, 5, 33, 35, 6),
    (37, 2, 59, 48, 39, 53),
)


def constants():
    steps = np.arange(TIMES, dtype=np.float64)
    columns = [np.ones_like(steps), (steps - (TIMES - 1) / 2.0) / (TIMES / 2.0)]
    for harmonic in range(1, 7):
        columns.append(np.cos(2.0 * np.pi * harmonic * steps / 12.0))
    for harmonic in range(1, 6):
        columns.append(np.sin(2.0 * np.pi * harmonic * steps / 12.0))
    columns.append(np.cos(2.0 * np.pi * steps / TIMES))
    columns.append(np.sin(2.0 * np.pi * steps / TIMES))
    columns.append(np.cos(4.0 * np.pi * steps / TIMES))
    basis = np.stack(columns, axis=1)
    others = (1, 13, 14, 15)
    gather = np.zeros((HARM, MONTHS + EXTRA))
    for row in range(HARM):
        if row in others:
            gather[row, MONTHS + others.index(row)] = 1.0
        else:
            gather[row, :MONTHS] = basis[:MONTHS, row]
    gram = basis.T @ basis
    fit = np.linalg.solve(gram, gather)
    root = np.linalg.cholesky(gather.T @ fit)
    table = basis[:, others]
    return table, fit, root


def flip(v, mask):
    if mask == 1:
        return v + 1 - 2 * lax.rem(v, 2)
    if mask == 3:
        return 3 - v
    return lax.rem(v + 2, 4)

def plan(flow):
    raw, _, post, _ = flow
    merged = {"zz": set(), "xx": {"x"}, "yxx": {"x", "y"}}[raw]
    values = {"zz": 8, "xx": 11, "yxx": 17}[raw]
    rows = []
    for axis in post:
        joins = axis in ("x", "y") and axis not in merged
        after = values
        if joins:
            after = values + (3 if not merged else 6)
        rows.append((axis, values, after, tuple(sorted(merged)), joins))
        if joins:
            merged.add(axis)
        values = after
    return rows


def flow_shapes(number):
    units = UNITS[number]
    rows = plan(FLOWS[number])
    if FLOWS[number][0] == "yxx":
        dims = {"r1": (2, 3, 4, 4), "r2": (2, 2, 3, 4), "r3": (2, 2, 3, 4)}
    else:
        dims = {"r1": (2, 2, 3, 4, 2), "r2": (2, 3, 4, 2)}
    blocks = (2,) * len(rows)
    dims["s0"] = blocks + (rows[0][1],)
    for at, (_, before, after, _, joins) in enumerate(rows):
        blocks = blocks[1:]
        dims[f"r{at + 6 - len(rows)}"] = blocks + (before,)
        if joins:
            dims[f"s{at + 1}"] = blocks + (after,)
    dims["out"] = (HARM + 1,)
    shapes = {name: (units,) + dim + (8, 128) for name, dim in dims.items()}
    if number in FIRST:
        shapes["stage"] = ((3, 4, 4) if FLOWS[number][0] == "yxx" else (2, 3, 4, 2)) + (8, 128)
    return shapes


def sent_tiles(number):
    rows = plan(FLOWS[number])
    return [48] * (5 - len(rows)) + [before << (len(rows) - 1 - at) for at, (_, before, *_) in enumerate(rows)]


def scratch():
    shapes = []
    for number in range(len(FLOWS)):
        for shape in flow_shapes(number).values():
            shapes.append(pltpu.VMEM(shape, jnp.float32))
    for units in POOL:
        shapes.append(pltpu.SemaphoreType.DMA((units,)))
    shapes.append(pltpu.SemaphoreType.DMA((STAGES,)))
    shapes.append(pltpu.SMEM((TIMES * EXTRA,), jnp.float32))
    shapes.append(pltpu.SemaphoreType.DMA(()))
    shapes.append(pltpu.SemaphoreType.DMA(()))
    shapes.append(pltpu.SemaphoreType.DMA((2, 2)))
    return shapes


def kernel(fit, root, table_hbm, x_ref, coef_ref, var_ref, *refs):
    me = lax.axis_index("io")
    core = lax.rem(me, 2)
    y = lax.rem(lax.div(me, 2), 2)
    x = lax.rem(lax.div(me, 4), 4)
    z = lax.div(me, 16)
    parity = lax.rem(x, 2)

    def dev(zz, xx, yy, cc):
        return ((zz * 4 + xx) * 2 + yy) * 2 + cc

    refs = list(refs)
    out_sem = refs.pop()
    stage_sem = refs.pop()
    table_sem = refs.pop()
    table_ref = refs.pop()
    send = refs.pop()
    table_copy = pltpu.make_async_copy(table_hbm, table_ref, table_sem)
    table_copy.start()
    flows = []
    at, base = 0, 0
    for number, spec in enumerate(FLOWS):
        raw, first, post, ring = spec
        flow = {"raw": raw, "f": first, "g": 4 - first, "post": post, "pf": ring, "pg": 4 - ring}
        flow["base"], flow["units"], flow["rows"] = base, UNITS[number], plan(spec)
        base += UNITS[number]
        for name in flow_shapes(number):
            flow[name] = refs[at]
            at += 1
        flow["swap"] = flow["base"] % 2 == 0 and UNITS[number] % 2 == 0
        flows.append(flow)
    for flow, pool in zip(flows, SEMS):
        flow["sem"] = {f"r{k + 1}": (refs[at + pool[k][0]], pool[k][1]) for k in range(5)}

    def arrival(flow, name, i):
        ref, length = flow["sem"][name]
        return ref.at[i if length == flow["units"] else lax.rem(i, length)]

    def push(src, dst, send, recv, device):
        pltpu.make_async_remote_copy(
            src_ref=src,
            dst_ref=dst,
            send_sem=send,
            recv_sem=recv,
            device_id={"io": device},
            device_id_type=pl.DeviceIdType.MESH,
        ).start()

    def await_bytes(ref, sem):
        pltpu.make_async_copy(ref, ref, sem).wait()

    barrier = pltpu.get_barrier_semaphore()
    friends = [dev(z, x, y, 1 - core), dev(z, x, 1 - y, core), dev(z, x, 1 - y, 1 - core)]
    for mask in (1, 3):
        for c in (core, 1 - core):
            friends.append(dev(flip(z, mask), x, y, c))
            friends.append(dev(z, flip(x, mask), y, c))
    for friend in friends:
        pl.semaphore_signal(barrier, inc=1, device_id={"io": friend}, device_id_type=pl.DeviceIdType.MESH)

    def place(flow, i, c):
        unit = flow["base"] + i
        half = lax.rem(i + 1 + c, 2) if flow["swap"] else lax.rem(unit, 2)
        return lax.div(unit, 2), half

    def begin_y(flow, i, mode=None):
        lat, half = place(flow, i, core)
        _, half_other = place(flow, i, 1 - core)
        for home, yy in ((1, 1 - y), (0, y)):
            for group, when in ((0, core), (2, core + 1), (1, 2 * core)):
                src = x_ref.at[group, lat, :, :, yy, half_other if group == 1 else half]
                dst = flow["r1"].at[i, home, when]
                recv = arrival(flow, "r1", i)
                c = 1 - core if group == 1 else core
                if mode == "fetch":
                    if home:
                        pltpu.make_async_copy(src, flow["stage"].at[group], stage_sem).start()
                elif home:
                    if mode == "staged":
                        src = flow["stage"].at[group]
                    push(src, dst, send.at[0], recv, dev(z, x, yy, c))
                elif group == 1:
                    push(src, dst, send.at[1], recv, dev(z, x, yy, c))
                else:
                    pltpu.make_async_copy(src, dst, recv).start()

    def second_y(flow, i):
        await_bytes(flow["r1"].at[i], arrival(flow, "r1", i))
        to = flip(x, flow["f"])
        for slot, block in ((1, flip(x, 2)), (0, to)):
            push(flow["r1"].at[i, :, :, :, block], flow["r2"].at[i, slot], send.at[2], arrival(flow, "r2", i), dev(z, to, y, core))

    def third_y(flow, i):
        await_bytes(flow["r2"].at[i], arrival(flow, "r2", i))
        to = flip(x, flow["g"])
        device = dev(z, to, y, core)
        push(flow["r1"].at[i, :, :, :, to], flow["r3"].at[i, 0], send.at[3], arrival(flow, "r3", i), device)
        push(flow["r2"].at[i, 1], flow["r3"].at[i, 1], send.at[3], arrival(flow, "r3", i), device)

    def begin(flow, i, mode=None):
        lat, half = place(flow, i, core)
        _, half_other = place(flow, i, 1 - core)
        along_z = flow["raw"] == "zz"
        here = z if along_z else x
        there = flip(here, flow["f"])
        for at_home in (False, True):
            spot = here if at_home else there
            zz, xx = (spot, x) if along_z else (z, spot)
            for slot, block in ((0, spot), (1, flip(spot, flow["g"]))):
                for group, when in ((0, core), (2, core + 1), (1, 2 * core)):
                    lon = half_other if group == 1 else half
                    if along_z:
                        src = x_ref.at[group, lat, block, :, :, lon]
                    else:
                        src = x_ref.at[group, lat, :, block, :, lon]
                    c = 1 - core if group == 1 else core
                    if mode == "fetch":
                        if not at_home:
                            pltpu.make_async_copy(src, flow["stage"].at[slot, group], stage_sem).start()
                    elif not at_home:
                        if mode == "staged":
                            src = flow["stage"].at[slot, group]
                        push(src, flow["r1"].at[i, 1, slot, when], send.at[0], arrival(flow, "r1", i), dev(zz, xx, y, c))
                    elif group == 1:
                        push(src, flow["r1"].at[i, 0, slot, when], send.at[1], arrival(flow, "r1", i), dev(zz, xx, y, c))
                    else:
                        pltpu.make_async_copy(src, flow["r1"].at[i, 0, slot, when], arrival(flow, "r1", i)).start()

    def second(flow, i):
        await_bytes(flow["r1"].at[i], arrival(flow, "r1", i))
        if flow["raw"] == "zz":
            to = dev(flip(z, flow["g"]), x, y, core)
        else:
            to = dev(z, flip(x, flow["g"]), y, core)
        push(flow["r1"].at[i, 0, 1], flow["r2"].at[i, 0], send.at[2], arrival(flow, "r2", i), to)
        push(flow["r1"].at[i, 1, 1], flow["r2"].at[i, 1], send.at[2], arrival(flow, "r2", i), to)

    def partner(flow, stage):
        axis = flow["post"][stage]
        if axis == "y":
            return dev(z, x, 1 - y, core)
        mask = flow["pg"] if axis in flow["post"][:stage] else flow["pf"]
        if axis == "x":
            return dev(z, flip(x, mask), y, core)
        return dev(flip(z, mask), x, y, core)

    def send_stats(flow, i, stage, state):
        step = stage + 6 - len(flow["rows"])
        name = f"r{step}"
        push(state.at[1], flow[name].at[i], send.at[step], arrival(flow, name, i), partner(flow, stage))

    def weights(chip, k):
        base = (chip * 3 + k) * EXTRA
        return [table_ref[base + j] for j in range(EXTRA)]

    def fold(pieces):
        sums, moments, total = {}, [None] * EXTRA, None
        for kind, k, value, chip in pieces:
            key = (kind, k)
            sums[key] = value if key not in sums else sums[key] + value
            w = weights(chip, k)
            for j in range(EXTRA):
                term = w[j] * value
                moments[j] = term if moments[j] is None else moments[j] + term
            square = value * value
            total = square if total is None else total + square
        return sums, moments, total

    def reduce_y(flow, i):
        await_bytes(flow["r3"].at[i], arrival(flow, "r3", i))
        r1, r2, r3, s0 = flow["r1"], flow["r2"], flow["r3"], flow["s0"]
        spots = (x, flip(x, flow["f"]), flip(x, flow["g"]), flip(x, 2))
        for b0 in (1, 0):
            for b1 in range(2):
                lon = (b0 * flow["pf"]) ^ (b1 * flow["pg"])
                block = z if lon == 0 else flip(z, lon)
                pieces = []
                for k in range(3):
                    for b, yy in enumerate((y, 1 - y)):
                        values = (r1[i, b, k, block, x], r2[i, 0, b, k, block], r3[i, 0, b, k, block], r3[i, 1, b, k, block])
                        for number, value in enumerate(values):
                            a = 0 if number in (0, 3) else 1
                            pieces.append(((a, b), k, value, z * 8 + spots[number] * 2 + yy))
                sums, moments, total = fold(pieces)
                for ((a, b), k), value in sums.items():
                    xl = 1 - parity if a else parity
                    yy = 1 - y if b else y
                    s0[i, b0, b1, 3 * (2 * xl + yy) + k] = value
                for j in range(EXTRA):
                    s0[i, b0, b1, MONTHS + j] = moments[j]
                s0[i, b0, b1, MONTHS + EXTRA] = total
        send_stats(flow, i, 0, s0.at[i])

    def reduce_raw(flow, i):
        await_bytes(flow["r2"].at[i], arrival(flow, "r2", i))
        r1, r2, s0 = flow["r1"], flow["r2"], flow["s0"]
        f, g, post = flow["f"], flow["g"], flow["post"]
        along_z = flow["raw"] == "zz"
        here = z if along_z else x
        spots = (here, flip(here, f), flip(here, g), flip(here, 2))
        chips = [spot * 8 + x * 2 + y if along_z else z * 8 + spot * 2 + y for spot in spots]
        across = x if along_z else z
        ring = "x" if along_z else "z"
        for b0 in (1, 0):
            for b1 in range(2):
                for b2 in range(2):
                    bits = (b0, b1, b2)
                    lon, lon_y, seen = 0, y, False
                    for bit, axis in zip(bits, post):
                        if axis == "y":
                            lon_y = 1 - y if bit else y
                        else:
                            lon = lon ^ (bit * (flow["pg"] if seen else flow["pf"]))
                            seen = True
                    block = across if lon == 0 else flip(across, lon)
                    pieces = []
                    for k in range(3):
                        values = (
                            r1[i, 0, 0, k, block, lon_y],
                            r1[i, 1, 0, k, block, lon_y],
                            r2[i, 0, k, block, lon_y],
                            r2[i, 1, k, block, lon_y],
                        )
                        for number, value in enumerate(values):
                            kind = 0 if along_z or number in (0, 3) else 1
                            pieces.append((kind, k, value, chips[number]))
                    sums, moments, total = fold(pieces)
                    for (a, k), value in sums.items():
                        if along_z:
                            s0[i, b0, b1, b2, k] = value
                        else:
                            s0[i, b0, b1, b2, 3 * (1 - parity if a else parity) + k] = value
                    months = 3 if along_z else 6
                    for j in range(EXTRA):
                        s0[i, b0, b1, b2, months + j] = moments[j]
                    s0[i, b0, b1, b2, months + EXTRA] = total
        send_stats(flow, i, 0, s0.at[i])

    def merge(flow, i, stage):
        name = f"r{stage + 6 - len(flow['rows'])}"
        await_bytes(flow[name].at[i], arrival(flow, name, i))
        axis, before, after, merged, joins = flow["rows"][stage]
        theirs = flow[name].at[i]
        mine = flow["state"].at[0]
        blocks = [()]
        for _ in range(len(flow["rows"]) - 1 - stage):
            blocks = [b + (bit,) for b in blocks for bit in (1, 0)]
        if not joins:
            for b in blocks:
                mine[b] = mine[b] + theirs[b]
            return mine
        new = flow[f"s{stage + 1}"].at[i]
        own_class = parity if axis == "x" else y
        months = before - EXTRA - 1
        for b in blocks:
            for k in range(months):
                if not merged:
                    spot = [3 * c + k for c in (own_class, 1 - own_class)]
                elif axis == "y":
                    spot = [6 * (k // 3) + 3 * c + k % 3 for c in (own_class, 1 - own_class)]
                else:
                    spot = [6 * c + k for c in (own_class, 1 - own_class)]
                new[b + (spot[0],)] = mine[b + (k,)]
                new[b + (spot[1],)] = theirs[b + (k,)]
            for j in range(EXTRA + 1):
                new[b + (2 * months + j,)] = mine[b + (months + j,)] + theirs[b + (months + j,)]
        return new

    def exchange(flow, i, stage):
        flow["state"] = flow["s0"].at[i]
        for done in range(stage - 1):
            joins = flow["rows"][done][4]
            flow["state"] = flow[f"s{done + 1}"].at[i] if joins else flow["state"].at[0]
        state = merge(flow, i, stage - 1)
        if stage < len(flow["rows"]):
            send_stats(flow, i, stage, state)
        return state

    def finish(flow, i):
        state = exchange(flow, i, len(flow["rows"]))
        out = flow["out"]
        w = [state[j] for j in range(MONTHS + EXTRA)]
        total = state[MONTHS + EXTRA]
        for row in range(HARM):
            value = None
            for j in range(MONTHS + EXTRA):
                term = w[j] * float(np.float32(fit[row, j]))
                value = term if value is None else value + term
            out[i, row] = value
        explained = None
        for col in range(HARM):
            value = None
            for j in range(col, HARM):
                if abs(root[j, col]) < 1e-12:
                    continue
                term = w[j] * float(np.float32(root[j, col]))
                value = term if value is None else value + term
            explained = value * value if explained is None else explained + value * value
        out[i, HARM] = (total - explained) * (1.0 / TIMES)
        lat, half = place(flow, i, core)
        row = core * 16 + lat

        @pl.when(half != core)
        def _():
            to = dev(z, x, y, 1 - core)
            push(out.at[i, 0:HARM], coef_ref.at[:, row], out_sem.at[0, 0], out_sem.at[1, 0], to)
            push(out.at[i, HARM], var_ref.at[row], out_sem.at[0, 1], out_sem.at[1, 1], to)

        @pl.when(half == core)
        def _():
            for k in range(HARM):
                coef_ref[k, row] = out[i, k]
            var_ref[row] = out[i, HARM]

    def step(flow, stage, i):
        early = (begin, second, reduce_raw)
        if flow["raw"] == "yxx":
            early = (begin_y, second_y, third_y, reduce_y)
        if stage < len(early):
            early[stage](flow, i)
        elif stage == 5:
            finish(flow, i)
        else:
            exchange(flow, i, stage + 1 - len(early))

    every = x_ref.reshape(3 * 16 * 64, 8, 128)

    def start(mode):
        for number in FIRST:
            (begin_y if flows[number]["raw"] == "yxx" else begin)(flows[number], core * 0, mode)

    start("fetch")
    pl.semaphore_wait(barrier, len(friends))
    await_bytes(every.at[pl.ds(0, 48 * len(FIRST))], stage_sem)
    start("staged")

    order = sorted((KEY[f][s], f, s) for f in range(len(FLOWS)) for s in range(STAGES))

    @pl.loop(0, max(u + max(d) for u, d in zip(UNITS, DELAY)))
    def _(turn):
        @pl.when(turn == min(d[5 - len(f["rows"])] for d, f in zip(DELAY, flows)))
        def _():
            table_copy.wait()

        for _, number, stage in order:
            flow = flows[number]
            unit = turn - DELAY[number][stage]

            lowest = 1 if stage == 0 and number in FIRST else 0

            @pl.when((unit >= lowest) & (unit < flow["units"]))
            def _(flow=flow, stage=stage, unit=unit):
                step(flow, stage, unit)

    totals = [sum(u * sent_tiles(n)[k] for n, u in enumerate(UNITS)) for k in range(5)]
    counts = [totals[0], 32 * 16] + totals[1:]
    for kind, count in enumerate(counts):
        await_bytes(every.at[pl.ds(0, count)], send.at[kind])
    for k in range(2):
        await_bytes(coef_ref.at[:, 0:16], out_sem.at[k, 0])
        await_bytes(var_ref.at[0:16], out_sem.at[k, 1])


def store(coef_vmem, var_vmem, coef_ref, var_ref, sems):
    copies = [pltpu.make_async_copy(coef_vmem.at[k], coef_ref.at[k], sems.at[k]) for k in range(HARM)]
    copies.append(pltpu.make_async_copy(var_vmem, var_ref, sems.at[HARM]))
    for copy in copies:
        copy.start()
    for copy in copies:
        copy.wait()


def local(snapshots):
    table, fit, root = constants()
    tiles = snapshots.reshape(48, 8, 64, 128).transpose(0, 2, 1, 3)
    tiles = tiles.reshape(3, 16, 4, 4, 2, 2, 8, 128)
    coeffs, variance = pl.pallas_call(
        functools.partial(kernel, fit, root),
        out_shape=(
            pltpu.VMEM((HARM, 32, 8, 128), jnp.float32),
            pltpu.VMEM((32, 8, 128), jnp.float32),
        ),
        in_specs=[pl.BlockSpec(memory_space=pl.ANY), pl.BlockSpec(memory_space=pl.ANY)],
        out_specs=(pl.BlockSpec(memory_space=pltpu.VMEM), pl.BlockSpec(memory_space=pltpu.VMEM)),
        scratch_shapes=scratch(),
        compiler_params=pltpu.CompilerParams(
            collective_id=0, has_side_effects=True, vmem_limit_bytes=VMEM_LIMIT
        ),
    )(jnp.asarray(table.reshape(-1), dtype=jnp.float32), tiles)
    coeffs, variance = pl.pallas_call(
        store,
        out_shape=(
            jax.ShapeDtypeStruct((HARM, 32, 8, 128), jnp.float32),
            jax.ShapeDtypeStruct((32, 8, 128), jnp.float32),
        ),
        in_specs=[pl.BlockSpec(memory_space=pltpu.VMEM)] * 2,
        out_specs=(pl.BlockSpec(memory_space=pl.ANY), pl.BlockSpec(memory_space=pl.ANY)),
        scratch_shapes=[pltpu.SemaphoreType.DMA((HARM + 1,))],
        compiler_params=pltpu.CompilerParams(vmem_limit_bytes=4 * 1024 * 1024),
    )(coeffs, variance)
    return coeffs.reshape(HARM, 256, 128), variance.reshape(256, 128)


def solution(mesh):
    return jax.shard_map(
        local,
        mesh=mesh,
        in_specs=(P(("rep", "io"), None),),
        out_specs=(P("rep", None, "io"), P("rep", "io")),
        check_vma=False,
    )
```

```python
import functools

import jax
import jax.numpy as jnp
import numpy as np
from jax import lax
from jax.experimental import pallas as pl
from jax.experimental.pallas import tpu as pltpu
from jax.sharding import PartitionSpec as P

TIMES = 96
HARM = 16
MONTHS = 12
EXTRA = 4
STAGES = 6
VMEM_LIMIT = 60817408
FLOWS = (
    ("zz", 3, "xyx", 3),
    ("zz", 1, "xyx", 1),
    ("xx", 1, "zzy", 1),
    ("xx", 3, "zzy", 3),
    ("xx", 1, "yzz", 1),
    ("xx", 3, "yzz", 3),
    ("zz", 1, "yxx", 1),
    ("zz", 3, "yxx", 3),
    ("yxx", 1, "zz", 1),
    ("yxx", 3, "zz", 3),
)
UNITS = (2, 2, 2, 2, 4, 4, 5, 5, 3, 3)
DELAY = (
    (4, 7, 9, 14, 17, 20),
    (3, 7, 10, 13, 16, 20),
    (3, 7, 9, 10, 16, 19),
    (0, 5, 7, 10, 12, 15),
    (0, 4, 5, 7, 14, 18),
    (2, 4, 5, 8, 14, 18),
    (0, 3, 6, 9, 13, 17),
    (0, 4, 6, 10, 13, 17),
    (1, 7, 9, 11, 15, 19),
    (1, 6, 7, 9, 14, 18),
)
FIRST = (7, 3, 6, 4, 8)
POOL = (5, 5, 5, 5, 5, 5, 4, 4, 4, 4, 4, 4, 3, 3, 2, 2, 2, 2, 2, 2, 2, 2, 2, 2)
SEMS = (
    ((15, 2), (18, 2), (8, 2), (20, 2), (3, 2)),
    ((17, 2), (19, 2), (16, 2), (21, 2), (14, 2)),
    ((16, 2), (20, 2), (14, 2), (17, 2), (22, 2)),
    ((14, 2), (21, 2), (22, 2), (23, 2), (15, 2)),
    ((6, 4), (9, 4), (8, 4), (1, 4), (7, 4)),
    ((7, 4), (10, 4), (11, 4), (6, 4), (11, 4)),
    ((0, 5), (2, 5), (4, 5), (2, 5), (0, 5)),
    ((1, 5), (3, 5), (5, 5), (3, 5), (4, 5)),
    ((12, 3), (7, 3), (13, 3), (12, 3), (9, 3)),
    ((13, 3), (0, 3), (9, 3), (10, 3), (5, 3)),
)
KEY = (
    (25, 44, 55, 12, 14, 9),
    (38, 56, 19, 17, 34, 40),
    (50, 29, 16, 30, 27, 7),
    (10, 45, 52, 15, 47, 20),
    (58, 11, 36, 23, 57, 43),
    (21, 22, 42, 49, 3, 13),
    (51, 24, 18, 46, 28, 8),
    (1, 0, 41, 26, 54, 4),
    (31, 32, 5, 33, 35, 6),
    (37, 2, 59, 48, 39, 53),
)


def constants():
    steps = np.arange(TIMES, dtype=np.float64)
    columns = [np.ones_like(steps), (steps - (TIMES - 1) / 2.0) / (TIMES / 2.0)]
    for harmonic in range(1, 7):
        columns.append(np.cos(2.0 * np.pi * harmonic * steps / 12.0))
    for harmonic in range(1, 6):
        columns.append(np.sin(2.0 * np.pi * harmonic * steps / 12.0))
    columns.append(np.cos(2.0 * np.pi * steps / TIMES))
    columns.append(np.sin(2.0 * np.pi * steps / TIMES))
    columns.append(np.cos(4.0 * np.pi * steps / TIMES))
    basis = np.stack(columns, axis=1)
    others = (1, 13, 14, 15)
    gather = np.zeros((HARM, MONTHS + EXTRA))
    for row in range(HARM):
        if row in others:
            gather[row, MONTHS + others.index(row)] = 1.0
        else:
            gather[row, :MONTHS] = basis[:MONTHS, row]
    gram = basis.T @ basis
    fit = np.linalg.solve(gram, gather)
    root = np.linalg.cholesky(gather.T @ fit)
    table = basis[:, others]
    return table, fit, root


def flip(v, mask):
    if mask == 1:
        return v + 1 - 2 * lax.rem(v, 2)
    if mask == 3:
        return 3 - v
    return lax.rem(v + 2, 4)

def plan(flow):
    raw, _, post, _ = flow
    merged = {"zz": set(), "xx": {"x"}, "yxx": {"x", "y"}}[raw]
    values = {"zz": 8, "xx": 11, "yxx": 17}[raw]
    rows = []
    for axis in post:
        joins = axis in ("x", "y") and axis not in merged
        after = values
        if joins:
            after = values + (3 if not merged else 6)
        rows.append((axis, values, after, tuple(sorted(merged)), joins))
        if joins:
            merged.add(axis)
        values = after
    return rows


def flow_shapes(number):
    units = UNITS[number]
    rows = plan(FLOWS[number])
    if FLOWS[number][0] == "yxx":
        dims = {"r1": (2, 3, 4, 4), "r2": (2, 2, 3, 4), "r3": (2, 2, 3, 4)}
    else:
        dims = {"r1": (2, 2, 3, 4, 2), "r2": (2, 3, 4, 2)}
    blocks = (2,) * len(rows)
    dims["s0"] = blocks + (rows[0][1],)
    for at, (_, before, after, _, joins) in enumerate(rows):
        blocks = blocks[1:]
        dims[f"r{at + 6 - len(rows)}"] = blocks + (before,)
        if joins:
            dims[f"s{at + 1}"] = blocks + (after,)
    dims["out"] = (HARM + 1,)
    shapes = {name: (units,) + dim + (8, 128) for name, dim in dims.items()}
    if number in FIRST:
        shapes["stage"] = ((3, 4, 4) if FLOWS[number][0] == "yxx" else (2, 3, 4, 2)) + (8, 128)
    return shapes


def sent_tiles(number):
    rows = plan(FLOWS[number])
    return [48] * (5 - len(rows)) + [before << (len(rows) - 1 - at) for at, (_, before, *_) in enumerate(rows)]


def scratch():
    shapes = []
    for number in range(len(FLOWS)):
        for shape in flow_shapes(number).values():
            shapes.append(pltpu.VMEM(shape, jnp.float32))
    for units in POOL:
        shapes.append(pltpu.SemaphoreType.DMA((units,)))
    shapes.append(pltpu.SemaphoreType.DMA((STAGES,)))
    shapes.append(pltpu.SMEM((TIMES * EXTRA,), jnp.float32))
    shapes.append(pltpu.SemaphoreType.DMA(()))
    shapes.append(pltpu.SemaphoreType.DMA(()))
    shapes.append(pltpu.SemaphoreType.DMA((2, 2)))
    return shapes


def kernel(fit, root, table_hbm, x_ref, coef_ref, var_ref, *refs):
    me = lax.axis_index("io")
    core = lax.rem(me, 2)
    y = lax.rem(lax.div(me, 2), 2)
    x = lax.rem(lax.div(me, 4), 4)
    z = lax.div(me, 16)
    parity = lax.rem(x, 2)

    def dev(zz, xx, yy, cc):
        return ((zz * 4 + xx) * 2 + yy) * 2 + cc

    refs = list(refs)
    out_sem = refs.pop()
    stage_sem = refs.pop()
    table_sem = refs.pop()
    table_ref = refs.pop()
    send = refs.pop()
    table_copy = pltpu.make_async_copy(table_hbm, table_ref, table_sem)
    table_copy.start()
    flows = []
    at, base = 0, 0
    for number, spec in enumerate(FLOWS):
        raw, first, post, ring = spec
        flow = {"raw": raw, "f": first, "g": 4 - first, "post": post, "pf": ring, "pg": 4 - ring}
        flow["base"], flow["units"], flow["rows"] = base, UNITS[number], plan(spec)
        base += UNITS[number]
        for name in flow_shapes(number):
            flow[name] = refs[at]
            at += 1
        flow["swap"] = flow["base"] % 2 == 0 and UNITS[number] % 2 == 0
        flows.append(flow)
    for flow, pool in zip(flows, SEMS):
        flow["sem"] = {f"r{k + 1}": (refs[at + pool[k][0]], pool[k][1]) for k in range(5)}

    def arrival(flow, name, i):
        ref, length = flow["sem"][name]
        return ref.at[i if length == flow["units"] else lax.rem(i, length)]

    def push(src, dst, send, recv, device):
        pltpu.make_async_remote_copy(
            src_ref=src,
            dst_ref=dst,
            send_sem=send,
            recv_sem=recv,
            device_id={"io": device},
            device_id_type=pl.DeviceIdType.MESH,
        ).start()

    def await_bytes(ref, sem):
        pltpu.make_async_copy(ref, ref, sem).wait()

    barrier = pltpu.get_barrier_semaphore()
    friends = [dev(z, x, y, 1 - core), dev(z, x, 1 - y, core), dev(z, x, 1 - y, 1 - core)]
    for mask in (3, 1):
        for c in (core, 1 - core):
            friends.append(dev(flip(z, mask), x, y, c))
            friends.append(dev(z, flip(x, mask), y, c))
    for friend in friends[3:] + friends[:3]:
        pl.semaphore_signal(barrier, inc=1, device_id={"io": friend}, device_id_type=pl.DeviceIdType.MESH)

    def place(flow, i, c):
        unit = flow["base"] + i
        half = lax.rem(i + 1 + c, 2) if flow["swap"] else lax.rem(unit, 2)
        return lax.div(unit, 2), half

    def begin_y(flow, i, mode=None):
        lat, half = place(flow, i, core)
        _, half_other = place(flow, i, 1 - core)
        for home, yy in ((1, 1 - y), (0, y)):
            for group, when in ((0, core), (2, core + 1), (1, 2 * core)):
                src = x_ref.at[group, lat, :, :, yy, half_other if group == 1 else half]
                dst = flow["r1"].at[i, home, when]
                recv = arrival(flow, "r1", i)
                c = 1 - core if group == 1 else core
                if mode == "fetch":
                    if home:
                        pltpu.make_async_copy(src, flow["stage"].at[group], stage_sem).start()
                elif home:
                    if mode == "staged":
                        src = flow["stage"].at[group]
                    push(src, dst, send.at[0], recv, dev(z, x, yy, c))
                elif group == 1:
                    push(src, dst, send.at[1], recv, dev(z, x, yy, c))
                else:
                    pltpu.make_async_copy(src, dst, recv).start()

    def second_y(flow, i):
        await_bytes(flow["r1"].at[i], arrival(flow, "r1", i))
        to = flip(x, flow["f"])
        for slot, block in ((1, flip(x, 2)), (0, to)):
            push(flow["r1"].at[i, :, :, :, block], flow["r2"].at[i, slot], send.at[2], arrival(flow, "r2", i), dev(z, to, y, core))

    def third_y(flow, i):
        await_bytes(flow["r2"].at[i], arrival(flow, "r2", i))
        to = flip(x, flow["g"])
        device = dev(z, to, y, core)
        push(flow["r1"].at[i, :, :, :, to], flow["r3"].at[i, 0], send.at[3], arrival(flow, "r3", i), device)
        push(flow["r2"].at[i, 1], flow["r3"].at[i, 1], send.at[3], arrival(flow, "r3", i), device)

    def begin(flow, i, mode=None):
        lat, half = place(flow, i, core)
        _, half_other = place(flow, i, 1 - core)
        along_z = flow["raw"] == "zz"
        here = z if along_z else x
        there = flip(here, flow["f"])
        for at_home in (False, True):
            spot = here if at_home else there
            zz, xx = (spot, x) if along_z else (z, spot)
            for slot, block in ((0, spot), (1, flip(spot, flow["g"]))):
                for group, when in ((0, core), (2, core + 1), (1, 2 * core)):
                    lon = half_other if group == 1 else half
                    if along_z:
                        src = x_ref.at[group, lat, block, :, :, lon]
                    else:
                        src = x_ref.at[group, lat, :, block, :, lon]
                    c = 1 - core if group == 1 else core
                    if mode == "fetch":
                        if not at_home:
                            pltpu.make_async_copy(src, flow["stage"].at[slot, group], stage_sem).start()
                    elif not at_home:
                        if mode == "staged":
                            src = flow["stage"].at[slot, group]
                        push(src, flow["r1"].at[i, 1, slot, when], send.at[0], arrival(flow, "r1", i), dev(zz, xx, y, c))
                    elif group == 1:
                        push(src, flow["r1"].at[i, 0, slot, when], send.at[1], arrival(flow, "r1", i), dev(zz, xx, y, c))
                    else:
                        pltpu.make_async_copy(src, flow["r1"].at[i, 0, slot, when], arrival(flow, "r1", i)).start()

    def second(flow, i):
        await_bytes(flow["r1"].at[i], arrival(flow, "r1", i))
        if flow["raw"] == "zz":
            to = dev(flip(z, flow["g"]), x, y, core)
        else:
            to = dev(z, flip(x, flow["g"]), y, core)
        push(flow["r1"].at[i, 0, 1], flow["r2"].at[i, 0], send.at[2], arrival(flow, "r2", i), to)
        push(flow["r1"].at[i, 1, 1], flow["r2"].at[i, 1], send.at[2], arrival(flow, "r2", i), to)

    def partner(flow, stage):
        axis = flow["post"][stage]
        if axis == "y":
            return dev(z, x, 1 - y, core)
        mask = flow["pg"] if axis in flow["post"][:stage] else flow["pf"]
        if axis == "x":
            return dev(z, flip(x, mask), y, core)
        return dev(flip(z, mask), x, y, core)

    def send_stats(flow, i, stage, state):
        step = stage + 6 - len(flow["rows"])
        name = f"r{step}"
        push(state.at[1], flow[name].at[i], send.at[step], arrival(flow, name, i), partner(flow, stage))

    def weights(chip, k):
        base = (chip * 3 + k) * EXTRA
        return [table_ref[base + j] for j in range(EXTRA)]

    def fold(pieces):
        sums, moments, total = {}, [None] * EXTRA, None
        for kind, k, value, chip in pieces:
            key = (kind, k)
            sums[key] = value if key not in sums else sums[key] + value
            w = weights(chip, k)
            for j in range(EXTRA):
                term = w[j] * value
                moments[j] = term if moments[j] is None else moments[j] + term
            square = value * value
            total = square if total is None else total + square
        return sums, moments, total

    def reduce_y(flow, i):
        await_bytes(flow["r3"].at[i], arrival(flow, "r3", i))
        r1, r2, r3, s0 = flow["r1"], flow["r2"], flow["r3"], flow["s0"]
        spots = (x, flip(x, flow["f"]), flip(x, flow["g"]), flip(x, 2))
        for b0 in (1, 0):
            for b1 in range(2):
                lon = (b0 * flow["pf"]) ^ (b1 * flow["pg"])
                block = z if lon == 0 else flip(z, lon)
                pieces = []
                for k in range(3):
                    for b, yy in enumerate((y, 1 - y)):
                        values = (r1[i, b, k, block, x], r2[i, 0, b, k, block], r3[i, 0, b, k, block], r3[i, 1, b, k, block])
                        for number, value in enumerate(values):
                            a = 0 if number in (0, 3) else 1
                            pieces.append(((a, b), k, value, z * 8 + spots[number] * 2 + yy))
                sums, moments, total = fold(pieces)
                for ((a, b), k), value in sums.items():
                    xl = 1 - parity if a else parity
                    yy = 1 - y if b else y
                    s0[i, b0, b1, 3 * (2 * xl + yy) + k] = value
                for j in range(EXTRA):
                    s0[i, b0, b1, MONTHS + j] = moments[j]
                s0[i, b0, b1, MONTHS + EXTRA] = total
        send_stats(flow, i, 0, s0.at[i])

    def reduce_raw(flow, i):
        await_bytes(flow["r2"].at[i], arrival(flow, "r2", i))
        r1, r2, s0 = flow["r1"], flow["r2"], flow["s0"]
        f, g, post = flow["f"], flow["g"], flow["post"]
        along_z = flow["raw"] == "zz"
        here = z if along_z else x
        spots = (here, flip(here, f), flip(here, g), flip(here, 2))
        chips = [spot * 8 + x * 2 + y if along_z else z * 8 + spot * 2 + y for spot in spots]
        across = x if along_z else z
        ring = "x" if along_z else "z"
        for b0 in (1, 0):
            for b1 in range(2):
                for b2 in range(2):
                    bits = (b0, b1, b2)
                    lon, lon_y, seen = 0, y, False
                    for bit, axis in zip(bits, post):
                        if axis == "y":
                            lon_y = 1 - y if bit else y
                        else:
                            lon = lon ^ (bit * (flow["pg"] if seen else flow["pf"]))
                            seen = True
                    block = across if lon == 0 else flip(across, lon)
                    pieces = []
                    for k in range(3):
                        values = (
                            r1[i, 0, 0, k, block, lon_y],
                            r1[i, 1, 0, k, block, lon_y],
                            r2[i, 0, k, block, lon_y],
                            r2[i, 1, k, block, lon_y],
                        )
                        for number, value in enumerate(values):
                            kind = 0 if along_z or number in (0, 3) else 1
                            pieces.append((kind, k, value, chips[number]))
                    sums, moments, total = fold(pieces)
                    for (a, k), value in sums.items():
                        if along_z:
                            s0[i, b0, b1, b2, k] = value
                        else:
                            s0[i, b0, b1, b2, 3 * (1 - parity if a else parity) + k] = value
                    months = 3 if along_z else 6
                    for j in range(EXTRA):
                        s0[i, b0, b1, b2, months + j] = moments[j]
                    s0[i, b0, b1, b2, months + EXTRA] = total
        send_stats(flow, i, 0, s0.at[i])

    def merge(flow, i, stage):
        name = f"r{stage + 6 - len(flow['rows'])}"
        await_bytes(flow[name].at[i], arrival(flow, name, i))
        axis, before, after, merged, joins = flow["rows"][stage]
        theirs = flow[name].at[i]
        mine = flow["state"].at[0]
        blocks = [()]
        for _ in range(len(flow["rows"]) - 1 - stage):
            blocks = [b + (bit,) for b in blocks for bit in (1, 0)]
        if not joins:
            for b in blocks:
                mine[b] = mine[b] + theirs[b]
            return mine
        new = flow[f"s{stage + 1}"].at[i]
        own_class = parity if axis == "x" else y
        months = before - EXTRA - 1
        for b in blocks:
            for k in range(months):
                if not merged:
                    spot = [3 * c + k for c in (own_class, 1 - own_class)]
                elif axis == "y":
                    spot = [6 * (k // 3) + 3 * c + k % 3 for c in (own_class, 1 - own_class)]
                else:
                    spot = [6 * c + k for c in (own_class, 1 - own_class)]
                new[b + (spot[0],)] = mine[b + (k,)]
                new[b + (spot[1],)] = theirs[b + (k,)]
            for j in range(EXTRA + 1):
                new[b + (2 * months + j,)] = mine[b + (months + j,)] + theirs[b + (months + j,)]
        return new

    def exchange(flow, i, stage):
        flow["state"] = flow["s0"].at[i]
        for done in range(stage - 1):
            joins = flow["rows"][done][4]
            flow["state"] = flow[f"s{done + 1}"].at[i] if joins else flow["state"].at[0]
        state = merge(flow, i, stage - 1)
        if stage < len(flow["rows"]):
            send_stats(flow, i, stage, state)
        return state

    def finish(flow, i):
        state = exchange(flow, i, len(flow["rows"]))
        out = flow["out"]
        w = [state[j] for j in range(MONTHS + EXTRA)]
        total = state[MONTHS + EXTRA]
        for row in range(HARM):
            value = None
            for j in range(MONTHS + EXTRA):
                term = w[j] * float(np.float32(fit[row, j]))
                value = term if value is None else value + term
            out[i, row] = value
        explained = None
        for col in range(HARM):
            value = None
            for j in range(col, HARM):
                if abs(root[j, col]) < 1e-12:
                    continue
                term = w[j] * float(np.float32(root[j, col]))
                value = term if value is None else value + term
            explained = value * value if explained is None else explained + value * value
        out[i, HARM] = (total - explained) * (1.0 / TIMES)
        lat, half = place(flow, i, core)
        row = core * 16 + lat

        @pl.when(half != core)
        def _():
            to = dev(z, x, y, 1 - core)
            push(out.at[i, 0:HARM], coef_ref.at[:, row], out_sem.at[0, 0], out_sem.at[1, 0], to)
            push(out.at[i, HARM], var_ref.at[row], out_sem.at[0, 1], out_sem.at[1, 1], to)

        @pl.when(half == core)
        def _():
            for k in range(HARM):
                coef_ref[k, row] = out[i, k]
            var_ref[row] = out[i, HARM]

    def step(flow, stage, i):
        early = (begin, second, reduce_raw)
        if flow["raw"] == "yxx":
            early = (begin_y, second_y, third_y, reduce_y)
        if stage < len(early):
            early[stage](flow, i)
        elif stage == 5:
            finish(flow, i)
        else:
            exchange(flow, i, stage + 1 - len(early))

    every = x_ref.reshape(3 * 16 * 64, 8, 128)

    def start(mode):
        for number in FIRST:
            (begin_y if flows[number]["raw"] == "yxx" else begin)(flows[number], core * 0, mode)

    start("fetch")
    pl.semaphore_wait(barrier, len(friends))
    await_bytes(every.at[pl.ds(0, 48 * len(FIRST))], stage_sem)
    start("staged")

    order = sorted((KEY[f][s], f, s) for f in range(len(FLOWS)) for s in range(STAGES))

    @pl.loop(0, max(u + max(d) for u, d in zip(UNITS, DELAY)))
    def _(turn):
        @pl.when(turn == min(d[5 - len(f["rows"])] for d, f in zip(DELAY, flows)))
        def _():
            table_copy.wait()

        for _, number, stage in order:
            flow = flows[number]
            unit = turn - DELAY[number][stage]

            lowest = 1 if stage == 0 and number in FIRST else 0

            @pl.when((unit >= lowest) & (unit < flow["units"]))
            def _(flow=flow, stage=stage, unit=unit):
                step(flow, stage, unit)

    totals = [sum(u * sent_tiles(n)[k] for n, u in enumerate(UNITS)) for k in range(5)]
    counts = [totals[0], 32 * 16] + totals[1:]
    for kind, count in enumerate(counts):
        await_bytes(every.at[pl.ds(0, count)], send.at[kind])
    for k in range(2):
        await_bytes(coef_ref.at[:, 0:16], out_sem.at[k, 0])
        await_bytes(var_ref.at[0:16], out_sem.at[k, 1])


def store(coef_vmem, var_vmem, coef_ref, var_ref, sems):
    copies = [pltpu.make_async_copy(var_vmem, var_ref, sems.at[4])]
    for k in range(4):
        rows = pl.ds(4 * k, 4)
        copies.append(pltpu.make_async_copy(coef_vmem.at[rows], coef_ref.at[rows], sems.at[k]))
    for copy in copies:
        copy.start()
    for copy in copies:
        copy.wait()


def local(snapshots):
    table, fit, root = constants()
    tiles = snapshots.reshape(48, 8, 64, 128).transpose(0, 2, 1, 3)
    tiles = tiles.reshape(3, 16, 4, 4, 2, 2, 8, 128)
    coeffs, variance = pl.pallas_call(
        functools.partial(kernel, fit, root),
        out_shape=(
            pltpu.VMEM((HARM, 32, 8, 128), jnp.float32),
            pltpu.VMEM((32, 8, 128), jnp.float32),
        ),
        in_specs=[pl.BlockSpec(memory_space=pl.ANY), pl.BlockSpec(memory_space=pl.ANY)],
        out_specs=(pl.BlockSpec(memory_space=pltpu.VMEM), pl.BlockSpec(memory_space=pltpu.VMEM)),
        scratch_shapes=scratch(),
        compiler_params=pltpu.CompilerParams(
            collective_id=0, has_side_effects=True, vmem_limit_bytes=VMEM_LIMIT
        ),
    )(jnp.asarray(table.reshape(-1), dtype=jnp.float32), tiles)
    coeffs, variance = pl.pallas_call(
        store,
        out_shape=(
            jax.ShapeDtypeStruct((HARM, 32, 8, 128), jnp.float32),
            jax.ShapeDtypeStruct((32, 8, 128), jnp.float32),
        ),
        in_specs=[pl.BlockSpec(memory_space=pltpu.VMEM)] * 2,
        out_specs=(pl.BlockSpec(memory_space=pl.ANY), pl.BlockSpec(memory_space=pl.ANY)),
        scratch_shapes=[pltpu.SemaphoreType.DMA((5,))],
        compiler_params=pltpu.CompilerParams(vmem_limit_bytes=4 * 1024 * 1024),
    )(coeffs, variance)
    return coeffs.reshape(HARM, 256, 128), variance.reshape(256, 128)


def solution(mesh):
    return jax.shard_map(
        local,
        mesh=mesh,
        in_specs=(P(("rep", "io"), None),),
        out_specs=(P("rep", None, "io"), P("rep", "io")),
        check_vma=False,
    )
```
